512 devices in a mesh: rad: 16 (over y_hi, z), ma: 32 (over y_lo, x, core).
Axes of the slice: x: 4, y: 8 (y_hi: 2, y_lo: 4; y = y_hi * 4 + y_lo), z: 8, core: 2. Of those that a mesh axis runs over, the one named last changes fastest.
Arguments:
- spectrum: bfloat16 [4, 512, 512, 384], P(None, 'ma', 'rad'), may hold values from -6 to 6
- radial_table: bfloat16 [12, 384], replicated, may hold values from -0.3125 to 0.3125
- legendre: bfloat16 [512, 512, 512], P('ma', 'rad'), may hold values from -0.375 to 0.375
- order_table: int32 [512], replicated, may hold values from 0 to 511, each once
- cylinder_row: int32 [512, 12], P(('rad', 'ma')), may hold values from 0 to 511
- column_weight: float32 [512, 12], P(('rad', 'ma')), may hold values from 0.5 to 2
Outputs:
- column_buoyancy: float32 [512, 1024], P('ma', 'rad')
- advected: float32 [2, 512, 12, 1024], P(None, ('rad', 'ma'))
The draws below stay inside these ranges and needn't reach their ends.
Inputs may be any that keep to these rules, and one draw needn't show every extreme that they name: `order_table`: each order appears in exactly one slot.
All inputs are finite; a program needn't handle non-finite values.
Results may differ from the reference program's by a relative error of at most 0.008.
Values may be sent and summed in bfloat16 or wider, within the bound.
No kernel may reach another device: no remote copies, remote signals or barrier semaphores. Data moves between devices by JAX's collectives and lax.ppermute only.
A program may use at most 64 MiB of HBM per device.

```python
import math
import jax
import jax.numpy as jnp
from jax import lax

L = 512
NCHEB = 384
NTH = 512
NPHI = 1024
NRAD = 12
NS = 512


def with_ends(drawn, stream_key, least, largest):
    longest = drawn.shape.index(max(drawn.shape))
    spots = []
    for shift in (0, 1):
        where = [jax.random.randint(jax.random.fold_in(stream_key, axis), (), 0, length) for axis, length in enumerate(drawn.shape)]
        where[longest] = (where[longest] + shift) % drawn.shape[longest]
        spots.append(tuple(where))
    return drawn.at[spots[0]].set(least).at[spots[1]].set(largest)


def shard_levels(key, dims, cuts, smallest, high):
    factor_of = 1.0
    for dim, parts in cuts:
        steps = jax.random.uniform(jax.random.fold_in(jax.random.fold_in(key, 6), dim), (parts,), jnp.float32, smallest / len(cuts), high / len(cuts))
        factor_of = factor_of * jnp.repeat(jnp.exp(steps), dims[dim] // parts).reshape((-1,) + (1,) * (len(dims) - 1 - dim))
    return factor_of


def centred(own_key, extent, spread, limit, cuts=(), held_as=jnp.bfloat16):
    values = jax.random.normal(own_key, extent, jnp.float32) * spread
    if len(cuts) > 0:
        values = shard_levels(own_key, extent, cuts, -0.22, 0.18) * values
    return jnp.clip(values, min=-limit, max=limit).astype(held_as)


def setup_inputs(seed: int = 0) -> dict:
    seeds = jax.random.split(jax.random.key(seed), 7)
    return {
        "spectrum": centred(seeds[0], (4, L, L, NCHEB), 1.0, 6.0, ((1, 32), (2, 16))),
        "radial_table": centred(seeds[1], (NRAD, NCHEB), NCHEB ** -0.5, 0.3125),
        "legendre": centred(seeds[2], (L, L, NTH), (L // 2) ** -0.5, 0.375, ((0, 32), (1, 16))),
        "order_table": jax.random.permutation(seeds[3], L).astype(jnp.int32),
        "cylinder_row": with_ends(jax.random.randint(seeds[4], (NTH, NRAD), 0, NS), jax.random.fold_in(seeds[4], 1), 0, NS - 1).astype(jnp.int32),
        "column_weight": jnp.clip(jnp.exp(math.log(2.0) - 1.3862944 * jax.random.uniform(seeds[5], (NTH, NRAD), jnp.float32) ** shard_levels(seeds[5], (NTH, NRAD), ((0, 512),), -0.2, 0.2)), 0.5, 2.0),
    }


def synthesis_tables(order_table):
    orders = order_table.astype(jnp.int32)
    longitude = jnp.arange(NPHI, dtype=jnp.int32)
    phase_index = orders[:, None] * longitude[None, :] % NPHI
    angles = phase_index.astype(jnp.float32) * (2.0 * math.pi / NPHI)
    weights = jnp.where(orders == 0, 1.0, 2.0).astype(jnp.float32) / math.sqrt(L)
    cosine = jnp.cos(angles) * weights[:, None]
    sine = jnp.sin(angles) * weights[:, None]
    slopes = (orders.astype(jnp.float32) / L)[:, None]
    values = jnp.stack([cosine, -sine])
    turned = jnp.stack([-sine * slopes, -cosine * slopes])
    return jnp.concatenate([values, turned], axis=2).astype(jnp.bfloat16)

def reference(spectrum, radial_table, legendre, order_table, cylinder_row, column_weight):

    def radial(block):
        flat_block = block.reshape(L * L, NCHEB)
        result = jnp.dot(flat_block, radial_table.T, preferred_element_type=jnp.float32)
        return jnp.moveaxis(result.astype(jnp.bfloat16).reshape(L, L, NRAD), 2, 0)
    levels = lax.map(radial, spectrum)
    degrees = jnp.arange(L, dtype=jnp.int32)

    def legendre_slot(operands):
        slot_table, slot_order, slot_coeff = operands
        allowed = (degrees >= slot_order)[:, None]
        masked = jnp.where(allowed, slot_table, jnp.zeros_like(slot_table))
        return jnp.dot(slot_coeff.reshape(4 * NRAD, L), masked, preferred_element_type=jnp.float32)
    sums = lax.map(legendre_slot, (legendre, order_table.astype(jnp.int32), jnp.moveaxis(levels, 2, 0)))
    latitudes = sums.astype(jnp.bfloat16).reshape(L, 2, 2, NRAD, NTH)
    tables = synthesis_tables(order_table)
    synthesis = jnp.einsum('kfirt,ikq->ftrq', latitudes.astype(jnp.float32), tables.astype(jnp.float32))
    synthesis = synthesis.astype(jnp.bfloat16)
    fields = synthesis[..., :NPHI].astype(jnp.float32)
    slope_field = synthesis[..., NPHI:].astype(jnp.float32)
    buoyancy = fields[0] - 0.8 * fields[1]
    weighted = (column_weight[:, :, None] * buoyancy).reshape(NTH * NRAD, NPHI)
    column = jax.ops.segment_sum(weighted, cylinder_row.reshape(-1), num_segments=NS)
    radius = 0.35 + 0.65 * (jnp.arange(NS, dtype=jnp.int32).astype(jnp.float32) + 0.5) / NS
    outward = (jnp.roll(column, -1, axis=1) - jnp.roll(column, 1, axis=1)) / (2.0 * radius[:, None])
    padded = jnp.pad(column, ((1, 1), (0, 0)))
    beside_all = -(padded[2:] - padded[:-2]) * 0.5
    velocity = jnp.stack([outward, beside_all]).astype(jnp.bfloat16).astype(jnp.float32)
    picked = velocity[:, cylinder_row]
    inverse = 1.0 / (0.35 + 0.65 * (cylinder_row.astype(jnp.float32) + 0.5) / NS)
    advected = fields - 0.05 * inverse[None, :, :, None] * (picked[1][None] * slope_field + picked[0][None] * fields)
    return (column, advected)
```

```python
import math

import jax
import jax.numpy as jnp
from jax import lax
from jax.sharding import PartitionSpec as P

NPHI = 1024
NS = 512
TIME_STEP = 0.05
COMPOSITION_WEIGHT = 0.8
BF16 = jnp.bfloat16
F32 = jnp.float32


def exchanged(blocks, axis):
    return lax.all_to_all(blocks, axis, split_axis=0, concat_axis=0, tiled=True)


def to_all(value, axis):
    return exchanged(jnp.broadcast_to(value, (lax.axis_size(axis), *value.shape)), axis)


def value_table(orders):
    longitude = jnp.arange(NPHI, dtype=jnp.int32)
    phase_index = orders[:, None] * longitude[None, :] % NPHI
    angles = phase_index.astype(F32) * (2.0 * math.pi / NPHI)
    weights = jnp.where(orders == 0, 1.0, 2.0).astype(F32) / math.sqrt(NS)
    return (
        (jnp.cos(angles) * weights[:, None]).astype(BF16),
        (-jnp.sin(angles) * weights[:, None]).astype(BF16),
    )


def on_device(spectrum, radial_table, legendre, order_table, cylinder_row, column_weight):
    slots, degrees = spectrum.shape[1:3]
    levels_n = radial_table.shape[0]
    lats = legendre.shape[2]
    n_rad = lax.axis_size("rad")
    n_ma = lax.axis_size("ma")
    lat_block = lats // n_rad
    row_block = NS // n_ma
    lon_block = NPHI // n_rad
    me_rad = lax.axis_index("rad")
    me_ma = lax.axis_index("ma")

    with jax.named_scope("contribute"):
        my_orders = lax.dynamic_slice_in_dim(order_table, me_ma * slots, slots)
        my_degrees = me_rad * degrees + jnp.arange(degrees, dtype=jnp.int32)
        allowed = my_degrees[None, :] >= my_orders[:, None]
        masked = jnp.where(allowed[:, :, None], legendre, jnp.zeros_like(legendre))
        levels = jnp.einsum(
            "rn,ckln->rckl", radial_table, spectrum, preferred_element_type=F32
        ).astype(BF16)
        contribution = jnp.einsum("klt,rckl->trck", masked, levels, preferred_element_type=F32)
        contribution = contribution.astype(BF16).reshape(n_rad, lat_block, levels_n * 4 * slots)
    with jax.named_scope("sum_degrees"):
        arrived = exchanged(contribution, "rad")
    with jax.named_scope("points"):
        info = jnp.concatenate([cylinder_row.astype(F32), column_weight], axis=1)
        infos = to_all(info, "ma").reshape(lat_block, 2 * levels_n)
        rows = infos[:, :levels_n].astype(jnp.int32).reshape(-1)
        weights = infos[:, levels_n:]
    with jax.named_scope("tables"):
        cosines, sines = value_table(order_table)
        table = jnp.stack(
            [cosines.reshape(n_ma, slots, NPHI), sines.reshape(n_ma, slots, NPHI)], axis=1
        )
    with jax.named_scope("latitudes"):
        latitudes = arrived.astype(F32).sum(axis=0).astype(BF16)
    with jax.named_scope("spread_orders"):
        received = exchanged(latitudes.reshape(n_ma, 1, -1), "ma")
    row_ids = jnp.arange(NS, dtype=jnp.int32)
    with jax.named_scope("columns"):
        lat32 = latitudes.astype(F32).reshape(lat_block, levels_n, 2, 2 * slots)
        weighted = (lat32[:, :, 0] - COMPOSITION_WEIGHT * lat32[:, :, 1]) * weights[:, :, None]
        onehot = (rows[:, None] == row_ids[None, :]).astype(F32)
        partial = jnp.einsum(
            "pq,ps->qs",
            weighted.reshape(-1, 2 * slots),
            onehot,
            precision=lax.Precision.HIGHEST,
            preferred_element_type=F32,
        )
    with jax.named_scope("sum_columns"):
        parts = to_all(partial.astype(BF16), "rad").reshape(n_rad, 2 * slots, NS)
        column = parts.astype(F32).sum(axis=0)
    with jax.named_scope("select"):
        step = jnp.sin(my_orders.astype(F32) * (2.0 * math.pi / NPHI))[:, None] * 2.0
        by_part = column.reshape(2, slots, NS)
        outward_hat = jnp.concatenate([-step * by_part[1], step * by_part[0]], axis=0)
        padded = jnp.pad(column, ((0, 0), (1, 1)))
        around_hat = padded[:, 2:] - padded[:, :-2]
        wanted = jnp.concatenate([outward_hat, around_hat, column], axis=0).astype(BF16)
        owned_rows = row_ids.reshape(n_ma, row_block)
        nothing = jnp.full((n_ma, row_block - levels_n), -1, jnp.int32)
        picks = jnp.concatenate([rows.reshape(n_ma, levels_n), nothing, owned_rows], axis=1)
        chooser = (picks.reshape(-1)[:, None] == row_ids[None, :]).astype(BF16)
        chosen = jnp.einsum("ps,qs->pq", chooser, wanted, preferred_element_type=F32).astype(BF16)
    with jax.named_scope("spread_columns"):
        got = exchanged(chosen.reshape(n_ma, 2 * row_block, 6 * slots), "ma")
    with jax.named_scope("synthesis"):
        coefs = received.reshape(n_ma, levels_n, 2, 2, slots)
        slope_scale = (order_table.astype(F32) / NS).reshape(n_ma, 1, 1, slots)
        c32 = coefs.astype(F32)
        slope_coefs = jnp.stack(
            [-c32[:, :, :, 1] * slope_scale, c32[:, :, :, 0] * slope_scale], axis=3
        ).astype(BF16)
        both = jnp.stack([coefs, slope_coefs], axis=1)
        grids = jnp.einsum("bgrfik,bikj->gfrj", both, table, preferred_element_type=F32)
        grids = grids.astype(BF16).astype(F32)
        fields, slope_field = grids[0], grids[1]
    with jax.named_scope("velocity"):
        got = got.reshape(n_ma, 2 * row_block, 3, 2, slots)
        synth = jnp.einsum("bpgik,bikj->gpj", got, table, preferred_element_type=F32)
        outward_diff = synth[0, :levels_n]
        around_diff = synth[1, :levels_n]
        owned = lax.dynamic_slice_in_dim(synth[2, row_block:], me_rad * lon_block, lon_block, axis=1)
    with jax.named_scope("advect"):
        radius = (0.35 + 0.65 * (cylinder_row.astype(F32) + 0.5) / NS).reshape(levels_n, 1)
        outward = outward_diff / (2.0 * radius)
        around = -0.5 * around_diff
        advected = fields - (TIME_STEP / radius) * (around * slope_field + outward * fields)
    return (owned, advected[:, None])


def solution(mesh):
    return jax.shard_map(
        on_device,
        mesh=mesh,
        in_specs=(
            P(None, "ma", "rad", None),
            P(),
            P("ma", "rad", None),
            P(),
            P(("rad", "ma"), None),
            P(("rad", "ma"), None),
        ),
        out_specs=(P("ma", "rad"), P(None, ("rad", "ma"), None, None)),
        check_vma=False,
    )
```

```python
import functools
import math

import jax
import jax.numpy as jnp
from jax import lax
from jax.experimental import pallas as pl
from jax.experimental.pallas import tpu as pltpu
from jax.sharding import PartitionSpec as P

NPHI = 1024
NS = 512
LANES = 128
TIME_STEP = 0.05
COMPOSITION_WEIGHT = 0.8
BF16 = jnp.bfloat16
F32 = jnp.float32
I32 = jnp.int32

dot = functools.partial(jnp.dot, preferred_element_type=F32)


def iota(shape, dim):
    return lax.broadcasted_iota(I32, shape, dim)


def dot_dims(x, y, dim_x, dim_y):
    return lax.dot_general(x, y, (((dim_x,), (dim_y,)), ((), ())), preferred_element_type=F32)


def vmem_call(body, outs, n_smem, n_vmem):
    return pl.pallas_call(
        body,
        out_shape=outs,
        in_specs=[pl.BlockSpec(memory_space=pltpu.SMEM)] * n_smem
        + [pl.BlockSpec(memory_space=pltpu.VMEM)] * n_vmem,
        out_specs=jax.tree.map(lambda _: pl.BlockSpec(memory_space=pltpu.VMEM), outs),
    )


def contribution_kernel(slots, degrees, orders, first, radial, spectrum, legendre, out):
    parts = spectrum.shape[0]
    levels_n = radial.shape[0]
    columns = levels_n * parts
    width = columns * slots
    rows = slots * degrees
    repeat = (iota((columns, levels_n), 0) // parts == iota((columns, levels_n), 1)).astype(BF16)
    repeated = dot(repeat, radial[...])
    part_of = iota(repeated.shape, 0) % parts
    levels = jnp.zeros((rows, columns), F32)
    for c in range(parts):
        table = jnp.where(part_of == c, repeated, 0.0).astype(BF16)
        levels += dot_dims(spectrum[c], table, 1, 1)
    spread = (iota((columns, width), 0) == iota((columns, width), 1) // slots).astype(BF16)
    expanded = dot(levels.astype(BF16), spread)
    slot_of_lane = iota((degrees, width), 1) % slots
    degree = iota((degrees, width), 0) + first[0]
    blocks = []
    for k in range(slots):
        kept = (slot_of_lane == k) & (degree >= orders[k])
        blocks.append(jnp.where(kept, expanded[k * degrees : (k + 1) * degrees], 0.0).astype(BF16))
    diagonal = jnp.concatenate(blocks, axis=0)
    total = dot_dims(legendre[...], diagonal, 0, 0)
    out[...] = total.astype(BF16).reshape(out.shape)


def column_kernel(arrived, weights, onehot, copies, stacked):
    levels_n = weights.shape[1]
    width = arrived.shape[2] // levels_n
    total = arrived[0].astype(F32)
    for d in range(1, arrived.shape[0]):
        total += arrived[d].astype(F32)
    points = jnp.concatenate(
        [total[:, r * width : (r + 1) * width] for r in range(levels_n)], axis=0
    ).astype(BF16)
    stacked[...] = jnp.concatenate([jnp.zeros_like(points), points], axis=1)
    half = width // 2
    exact = points.astype(F32)
    buoyancy = exact[:, :half] - COMPOSITION_WEIGHT * exact[:, half:]
    weight = jnp.concatenate([weights[:, r : r + 1] for r in range(levels_n)], axis=0)
    weighted = buoyancy * weight
    high = weighted.astype(BF16)
    low = (weighted - high.astype(F32)).astype(BF16)
    both = dot_dims(jnp.concatenate([high, low], axis=1), onehot[...], 0, 0)
    column = (both[:half] + both[half:]).astype(BF16)
    copies[...] = jnp.broadcast_to(column[None], copies.shape)


def select_kernel(parts, step, chooser, stacked, out):
    column = parts[0].astype(F32)
    for d in range(1, parts.shape[0]):
        column += parts[d].astype(F32)
    half = column.shape[0] // 2
    outward = step[...] * jnp.concatenate([column[half:], column[:half]], axis=0)
    at = iota(column.shape, 1)
    after = jnp.where(at == NS - 1, 0.0, pltpu.roll(column, NS - 1, axis=1))
    before = jnp.where(at == 0, 0.0, pltpu.roll(column, 1, axis=1))
    around = after - before
    zeros = jnp.zeros_like(column)
    points = jnp.concatenate([outward, around, zeros, zeros], axis=0).astype(BF16)
    group = at // 4 % 4
    rows = jnp.concatenate([jnp.where(group == g, column, 0.0) for g in range(4)], axis=0)
    chosen = dot_dims(chooser[:, :NS], points, 1, 1)
    chosen += dot_dims(chooser[:, NS : 2 * NS], rows.astype(BF16), 1, 1)
    chosen += dot(chooser[:, 2 * NS :], stacked[...])
    out[...] = chosen.astype(BF16).reshape(out.shape)


def advect_kernel(levels_n, slots, block, got, cosines, sines, slope, radius, owned, advected):
    n_ma, per, _ = got.shape
    taken = [got[b] for b in range(n_ma)]
    by_part = []
    for i in range(2):
        groups = []
        for g in range(4):
            at = (2 * g + i) * slots
            groups.append(jnp.concatenate([x[:, at : at + slots] for x in taken], axis=1))
        by_part.append(groups)
    scale = slope[...]
    sides = []
    for i in range(2):
        turned = [
            (by_part[1 - i][g].astype(F32) * (scale if i else -scale)).astype(BF16) for g in (2, 3)
        ]
        sides.append(jnp.concatenate(by_part[i] + turned, axis=0))
    result = dot(sides[0], cosines[...]) + dot(sides[1], sines[...])
    rows = [result[g * per : g * per + levels_n] for g in range(6)]
    inverse = 1.0 / radius[...]
    outward = rows[0] * (0.5 * inverse)
    around = -0.5 * rows[1]
    held = [x.astype(BF16).astype(F32) for x in rows[2:]]
    for f in range(2):
        field, side = held[f], held[2 + f]
        advected[f] = field - (TIME_STEP * inverse) * (around * side + outward * field)
    mine = jnp.concatenate([result[g * per + levels_n : (g + 1) * per] for g in range(4)], axis=0)
    width = owned.shape[1]
    mine = pltpu.roll(mine, lax.rem(NPHI - block[0], NPHI), axis=1)
    owned[...] = mine[:, :width]


def exchanged(blocks, axis):
    return lax.all_to_all(blocks, axis, split_axis=0, concat_axis=0, tiled=True)


def value_tables(orders):
    longitude = jnp.arange(NPHI, dtype=I32)
    phase_index = orders[:, None] * longitude[None, :] % NPHI
    angles = phase_index.astype(F32) * (2.0 * math.pi / NPHI)
    weights = jnp.where(orders == 0, 1.0, 2.0).astype(F32) / math.sqrt(NS)
    return (
        (jnp.cos(angles) * weights[:, None]).astype(BF16),
        (-jnp.sin(angles) * weights[:, None]).astype(BF16),
    )


def choosers(rows, n_ma, levels_n, per):
    q = jnp.arange(per, dtype=I32)[None, :, None]
    b = jnp.arange(n_ma, dtype=I32)[:, None, None]
    s = jnp.arange(NS, dtype=I32)[None, None, :]
    p = jnp.arange(levels_n * n_ma, dtype=I32)[None, None, :]
    padded = jnp.pad(rows, ((0, 0), (0, per - levels_n)), constant_values=-1)
    point = padded[:, :, None] == s
    owned = (s // per == b) & (q >= levels_n) & (s % (per - levels_n) == q - levels_n)
    latitude = (p % n_ma == b) & (p // n_ma == q)
    return jnp.concatenate([point, owned, latitude], axis=2).astype(BF16).reshape(n_ma * per, -1)


def on_device(spectrum, radial_table, legendre, order_table, cylinder_row, column_weight):
    parts, slots, degrees, modes = spectrum.shape
    levels_n = radial_table.shape[0]
    lats = legendre.shape[2]
    n_rad = lax.axis_size("rad")
    n_ma = lax.axis_size("ma")
    lat_block = lats // n_rad
    row_block = NS // n_ma
    lon_block = NPHI // n_rad
    me_rad = lax.axis_index("rad")
    me_ma = lax.axis_index("ma")
    my_orders = lax.dynamic_slice_in_dim(order_table, me_ma * slots, slots)

    info = jnp.concatenate([cylinder_row.astype(F32), column_weight], axis=1)
    infos = exchanged(jnp.broadcast_to(info, (n_ma, 1, 2 * levels_n)), "ma")
    infos = infos.reshape(n_ma, 2 * levels_n)
    rows = infos[:, :levels_n].astype(I32)
    weights = infos[:, levels_n:]
    first = (me_rad * degrees).astype(I32).reshape(1)
    contribution = vmem_call(
        functools.partial(contribution_kernel, slots, degrees),
        jax.ShapeDtypeStruct((n_rad, lat_block, levels_n * parts * slots), BF16),
        2, 3,
    )(
        my_orders,
        first,
        radial_table,
        spectrum.reshape(parts, slots * degrees, modes),
        legendre.reshape(slots * degrees, lats),
    )
    arrived = exchanged(contribution, "rad")
    cosines, sines = value_tables(order_table)
    row_ids = jnp.arange(NS, dtype=I32)
    onehot = (rows.T.reshape(-1)[:, None] == row_ids[None, :]).astype(BF16)
    chooser = choosers(rows, n_ma, levels_n, row_block)
    step = 2.0 * jnp.sin(my_orders.astype(F32) * (2.0 * math.pi / NPHI))
    step = jnp.concatenate([-step, step]).reshape(2 * slots, 1)
    slope = (order_table.astype(F32) / NS).reshape(1, -1)
    radius = (0.35 + 0.65 * (cylinder_row.astype(F32) + 0.5) / NS).reshape(levels_n, 1)
    copies, stacked = vmem_call(
        column_kernel,
        (
            jax.ShapeDtypeStruct((n_rad, 2 * slots, NS), BF16),
            jax.ShapeDtypeStruct((levels_n * lat_block, LANES), BF16),
        ),
        0, 3,
    )(arrived, weights, onehot)
    partials = exchanged(copies, "rad")
    chosen = vmem_call(
        select_kernel,
        jax.ShapeDtypeStruct((n_ma, row_block, LANES), BF16),
        0, 4,
    )(partials, step, chooser, stacked)
    got = exchanged(chosen, "ma")
    owned, advected = vmem_call(
        functools.partial(advect_kernel, levels_n, slots),
        (
            jax.ShapeDtypeStruct((row_block, lon_block), F32),
            jax.ShapeDtypeStruct((2, levels_n, NPHI), F32),
        ),
        1, 5,
    )((me_rad * lon_block).astype(I32).reshape(1), got, cosines, sines, slope, radius)
    return (owned, advected[:, None])


def solution(mesh):
    return jax.shard_map(
        on_device,
        mesh=mesh,
        in_specs=(
            P(None, "ma", "rad", None),
            P(),
            P("ma", "rad", None),
            P(),
            P(("rad", "ma"), None),
            P(("rad", "ma"), None),
        ),
        out_specs=(P("ma", "rad"), P(None, ("rad", "ma"), None, None)),
        check_vma=False,
    )
```

```python
import functools
import math

import jax
import jax.numpy as jnp
from jax import lax
from jax.experimental import pallas as pl
from jax.experimental.pallas import tpu as pltpu
from jax.sharding import Mesh
from jax.sharding import PartitionSpec as P

NPHI = 1024
NS = 512
LANES = 128
HALVES = 2
VMEM_LIMIT = 20 * 2**20
TIME_STEP = 0.05
COMPOSITION_WEIGHT = 0.8
BF16 = jnp.bfloat16
F32 = jnp.float32
I32 = jnp.int32

dot = functools.partial(jnp.dot, preferred_element_type=F32)


def iota(shape, dim):
    return lax.broadcasted_iota(I32, shape, dim)


def as_column(row, width):
    return jnp.transpose(jnp.broadcast_to(row, (8, width)))[:, :1]


def matches(column, row):
    return (column == row).astype(F32).astype(BF16)


def dot_dims(x, y, dim_x, dim_y):
    return lax.dot_general(x, y, (((dim_x,), (dim_y,)), ((), ())), preferred_element_type=F32)


def vmem_call(body, outs, n_smem, n_vmem):
    return pl.pallas_call(
        body,
        out_shape=outs,
        in_specs=[pl.BlockSpec(memory_space=pltpu.SMEM)] * n_smem
        + [pl.BlockSpec(memory_space=pltpu.VMEM)] * n_vmem,
        out_specs=jax.tree.map(lambda _: pl.BlockSpec(memory_space=pltpu.VMEM), outs),
        compiler_params=pltpu.CompilerParams(vmem_limit_bytes=VMEM_LIMIT),
    )


def contribution_kernel(slots, degrees, halves, orders, first, radial, spectrum, legendre, out):
    parts = spectrum.shape[0]
    levels_n = radial.shape[0]
    columns = levels_n * parts
    width = columns * slots
    rows = slots * degrees
    repeat = (iota((columns, levels_n), 0) // parts == iota((columns, levels_n), 1)).astype(BF16)
    repeated = dot(repeat, radial[...])
    part_of = iota(repeated.shape, 0) % parts
    levels = jnp.zeros((rows, columns), F32)
    for c in range(parts):
        table = jnp.where(part_of == c, repeated, 0.0).astype(BF16)
        levels += dot_dims(spectrum[c], table, 1, 1)
    spread = (iota((columns, width), 0) == iota((columns, width), 1) // slots).astype(BF16)
    expanded = dot(levels.astype(BF16), spread)
    slot_of_lane = iota((degrees, width), 1) % slots
    degree = iota((degrees, width), 0) + first[0]
    blocks = []
    for k in range(slots):
        kept = (slot_of_lane == k) & (degree >= orders[k])
        blocks.append(jnp.where(kept, expanded[k * degrees : (k + 1) * degrees], 0.0).astype(BF16))
    diagonal = jnp.concatenate(blocks, axis=0)
    total = dot_dims(legendre[...], diagonal, 0, 0).astype(BF16)
    n_z, lats, _ = out.shape
    block = lats // halves
    for h in range(halves):
        for z in range(n_z):
            at = (h * n_z + z) * block
            out[z, h * block : (h + 1) * block] = total[at : at + block]


def column_kernel(arrived, weights, rows, copies, stacked):
    levels_n = weights.shape[1]
    width = arrived.shape[2] // levels_n
    total = arrived[0].astype(F32)
    for d in range(1, arrived.shape[0]):
        total += arrived[d].astype(F32)
    points = jnp.concatenate(
        [total[:, r * width : (r + 1) * width] for r in range(levels_n)], axis=0
    ).astype(BF16)
    stacked[...] = jnp.concatenate([jnp.zeros_like(points), points], axis=1)
    half = width // 2
    exact = points.astype(F32)
    buoyancy = exact[:, :half] - COMPOSITION_WEIGHT * exact[:, half:]
    weight = jnp.concatenate([weights[:, r : r + 1] for r in range(levels_n)], axis=0)
    weighted = buoyancy * weight
    high = weighted.astype(BF16)
    low = (weighted - high.astype(F32)).astype(BF16)
    count = rows.shape[1]
    onehot = matches(as_column(rows[...], count), iota((count, NS), 1))
    both = dot_dims(jnp.concatenate([high, low], axis=1), onehot, 0, 0)
    column = (both[:half] + both[half:]).astype(BF16)
    copies[...] = jnp.broadcast_to(column[None], copies.shape)


def message_kernel(per, stacked, base):
    lats = base.shape[0] // per
    count = stacked.shape[0]
    point = iota((1, count), 1)
    code = point % lats * per + point // lats
    base[...] = dot(matches(iota((lats * per, count), 0), code), stacked[...]).astype(BF16)


def select_kernel(levels_n, parts, step, picks, base, out):
    column = parts[0].astype(F32)
    for d in range(1, parts.shape[0]):
        column += parts[d].astype(F32)
    half = column.shape[0] // 2
    outward = step[...] * jnp.concatenate([column[half:], column[:half]], axis=0)
    at = iota(column.shape, 1)
    after = jnp.where(at == NS - 1, 0.0, pltpu.roll(column, NS - 1, axis=1))
    before = jnp.where(at == 0, 0.0, pltpu.roll(column, 1, axis=1))
    around = after - before
    zeros = jnp.zeros_like(column)
    points = jnp.concatenate([outward, around, zeros, zeros], axis=0).astype(BF16)
    group = at // 4 % 4
    rows = jnp.concatenate([jnp.where(group == g, column, 0.0) for g in range(4)], axis=0)
    per = out.shape[1]
    own = per - levels_n
    count = picks.shape[1]
    s = iota((1, NS), 1)
    n_ma = NS // per
    message = iota((count, 1), 0)
    q = message % per
    code = jnp.where(q >= levels_n, message // per % n_ma * own + q - levels_n, -1)
    chosen = dot_dims(matches(as_column(picks[...], count), s), points, 1, 1)
    chosen += dot_dims(matches(code, s // per * own + s % own), rows.astype(BF16), 1, 1)
    chosen += base[...].astype(F32)
    out[...] = chosen.astype(BF16).reshape(out.shape)


def advect_kernel(levels_n, slots, block, got, cosines, sines, slope, radius, owned, advected):
    n_ma, per, _ = got.shape[1:]
    taken = [(got[0, b].astype(F32) + got[1, b].astype(F32)).astype(BF16) for b in range(n_ma)]
    by_part = []
    for i in range(2):
        groups = []
        for g in range(4):
            at = (2 * g + i) * slots
            groups.append(jnp.concatenate([x[:, at : at + slots] for x in taken], axis=1))
        by_part.append(groups)
    scale = slope[...]
    sides = []
    for i in range(2):
        turned = [
            (by_part[1 - i][g].astype(F32) * (scale if i else -scale)).astype(BF16) for g in (2, 3)
        ]
        sides.append(jnp.concatenate(by_part[i] + turned, axis=0))
    result = dot(sides[0], cosines[...]) + dot(sides[1], sines[...])
    rows = [result[g * per : g * per + levels_n] for g in range(6)]
    inverse = 1.0 / radius[...]
    outward = rows[0] * (0.5 * inverse)
    around = -0.5 * rows[1]
    held = [x.astype(BF16).astype(F32) for x in rows[2:]]
    for f in range(2):
        field, side = held[f], held[2 + f]
        value = field - (TIME_STEP * inverse) * (around * side + outward * field)
        for r in range(levels_n):
            advected[f, r] = value[r : r + 1]
    mine = jnp.concatenate([result[g * per + levels_n : (g + 1) * per] for g in range(4)], axis=0)
    width = owned.shape[1]
    mine = pltpu.roll(mine, lax.rem(NPHI - block[0], NPHI), axis=1)
    owned[...] = mine[:, :width]


def exchanged(blocks, axis):
    return lax.all_to_all(blocks, axis, split_axis=0, concat_axis=0, tiled=True)


def value_tables(orders):
    longitude = jnp.arange(NPHI, dtype=I32)
    phase_index = orders[:, None] * longitude[None, :] % NPHI
    angles = phase_index.astype(F32) * (2.0 * math.pi / NPHI)
    weights = jnp.where(orders == 0, 1.0, 2.0).astype(F32) / math.sqrt(NS)
    return (
        (jnp.cos(angles) * weights[:, None]).astype(BF16),
        (-jnp.sin(angles) * weights[:, None]).astype(BF16),
    )


def on_device(spectrum, radial_table, legendre, order_table, cylinder_row, column_weight):
    parts, slots, degrees, modes = spectrum.shape
    levels_n = radial_table.shape[0]
    lats = legendre.shape[2]
    n_z = lax.axis_size("z")
    n_half = lax.axis_size("half")
    n_ma = lax.axis_size("ma")
    lat_block = lats // n_z
    row_block = NS // n_ma
    lon_block = NPHI // (n_half * n_z)
    me_rad = lax.axis_index(("half", "z"))
    me_ma = lax.axis_index("ma")
    my_orders = lax.dynamic_slice_in_dim(order_table, me_ma * slots, slots)

    info = jnp.concatenate([cylinder_row.astype(F32), column_weight], axis=1)
    infos = exchanged(
        jnp.broadcast_to(info, (lat_block, 1, 2 * levels_n)), ("half", "ma")
    ).reshape(lat_block, 2 * levels_n)
    rows = infos[:, :levels_n].astype(I32)
    weights = infos[:, levels_n:]
    first = (me_rad * degrees).astype(I32).reshape(1)
    contribution = vmem_call(
        functools.partial(contribution_kernel, slots, degrees, n_half),
        pltpu.HBM((n_z, lat_block, levels_n * parts * slots), BF16),
        2, 3,
    )(
        my_orders,
        first,
        radial_table,
        spectrum.reshape(parts, slots * degrees, modes),
        legendre.reshape(slots * degrees, lats),
    )
    arrived = exchanged(contribution, "z")
    cosines, sines = value_tables(order_table)
    point_rows = rows.T.reshape(1, -1)
    picks = jnp.pad(rows, ((0, 0), (0, row_block - levels_n)), constant_values=-1)
    picks = picks.reshape(1, -1)
    step = 2.0 * jnp.sin(my_orders.astype(F32) * (2.0 * math.pi / NPHI))
    step = jnp.concatenate([-step, step]).reshape(2 * slots, 1)
    slope = (order_table.astype(F32) / NS).reshape(1, -1)
    radius = (0.35 + 0.65 * (cylinder_row.astype(F32) + 0.5) / NS).reshape(levels_n, 1)
    copies, stacked = vmem_call(
        column_kernel,
        (
            pltpu.HBM((n_z, 2 * slots, NS), BF16),
            jax.ShapeDtypeStruct((levels_n * lat_block, LANES), BF16),
        ),
        0, 3,
    )(arrived, weights, point_rows)
    partials = exchanged(copies, "z")
    base = vmem_call(
        functools.partial(message_kernel, row_block),
        jax.ShapeDtypeStruct((lat_block * row_block, LANES), BF16),
        0, 1,
    )(stacked)
    chosen = vmem_call(
        functools.partial(select_kernel, levels_n),
        pltpu.HBM((lat_block, row_block, LANES), BF16),
        0, 4,
    )(partials, step, picks, base)
    got = exchanged(chosen, ("half", "ma")).reshape(n_half, n_ma, row_block, LANES)
    owned, advected = vmem_call(
        functools.partial(advect_kernel, levels_n, slots),
        (
            jax.ShapeDtypeStruct((row_block, lon_block), F32),
            jax.ShapeDtypeStruct((2, levels_n, 1, NPHI), F32),
        ),
        1, 5,
    )((me_rad * lon_block).astype(I32).reshape(1), got, cosines, sines, slope, radius)
    return (owned, jnp.swapaxes(advected, 1, 2))


def solution(mesh):
    parts = Mesh(mesh.devices.reshape(HALVES, -1, mesh.shape["ma"]), ("half", "z", "ma"))
    rad = ("half", "z")
    return jax.shard_map(
        on_device,
        mesh=parts,
        in_specs=(
            P(None, "ma", rad, None),
            P(),
            P("ma", rad, None),
            P(),
            P((*rad, "ma"), None),
            P((*rad, "ma"), None),
        ),
        out_specs=(P("ma", rad), P(None, (*rad, "ma"), None, None)),
        check_vma=False,
    )
```

```python
import functools
import math

import jax
import jax.numpy as jnp
from jax import lax
from jax.experimental import pallas as pl
from jax.experimental.pallas import tpu as pltpu
from jax.sharding import Mesh
from jax.sharding import PartitionSpec as P

NPHI = 1024
NS = 512
LANES = 128
HALVES = 2
PAIRS = 2
MA = ("pair", "y", "x", "core")
VMEM_LIMIT = 20 * 2**20
TIME_STEP = 0.05
COMPOSITION_WEIGHT = 0.8
BF16 = jnp.bfloat16
F32 = jnp.float32
I32 = jnp.int32

dot = functools.partial(jnp.dot, preferred_element_type=F32)


def iota(shape, dim):
    return lax.broadcasted_iota(I32, shape, dim)


def as_column(row, width):
    return jnp.transpose(jnp.broadcast_to(row, (8, width)))[:, :1]


def matches(column, row):
    return (column == row).astype(F32).astype(BF16)


def dot_dims(x, y, dim_x, dim_y):
    return lax.dot_general(x, y, (((dim_x,), (dim_y,)), ((), ())), preferred_element_type=F32)


def vmem_call(body, outs, n_smem, n_vmem, n_hbm=0, scratch=()):
    return pl.pallas_call(
        body,
        out_shape=outs,
        in_specs=[pl.BlockSpec(memory_space=pltpu.SMEM)] * n_smem
        + [pl.BlockSpec(memory_space=pltpu.VMEM)] * n_vmem
        + [pl.BlockSpec(memory_space=pltpu.HBM)] * n_hbm,
        out_specs=jax.tree.map(lambda _: pl.BlockSpec(memory_space=pltpu.VMEM), outs),
        scratch_shapes=scratch,
        compiler_params=pltpu.CompilerParams(vmem_limit_bytes=VMEM_LIMIT),
    )


def info_kernel(rows, weights, out):
    info = jnp.concatenate([rows[...].astype(F32), weights[...]], axis=1)
    for d in range(out.shape[0]):
        out[d] = info


def in_place(infos):
    count = infos.shape[0] // 4
    pieces = [infos[j * count : (j + 1) * count] for j in range(4)]
    pair, half = lax.axis_index("pair") == 0, lax.axis_index("half") == 0
    halves = [
        jnp.concatenate([jnp.where(pair, a, b), jnp.where(pair, b, a)], axis=0)
        for a, b in (pieces[:2], pieces[2:])
    ]
    a, b = halves
    return jnp.concatenate([jnp.where(half, a, b), jnp.where(half, b, a)], axis=0)


def contribution_kernel(
    slots, degrees, halves, orders, radial, spectrum_in, legendre_in, out, spectrum, legendre, sems
):
    parts = spectrum.shape[0]
    copies = [
        pltpu.make_async_copy(spectrum_in.at[c], spectrum.at[c], sems.at[c]) for c in range(parts)
    ]
    copies.append(pltpu.make_async_copy(legendre_in, legendre, sems.at[parts]))
    for copy in copies:
        copy.start()
    levels_n = radial.shape[0]
    columns = levels_n * parts
    width = columns * slots
    rows = slots * degrees
    repeat = (iota((columns, levels_n), 0) // parts == iota((columns, levels_n), 1)).astype(BF16)
    repeated = dot(repeat, radial[...])
    part_of = iota(repeated.shape, 0) % parts
    levels = jnp.zeros((rows, columns), F32)
    for c in range(parts):
        table = jnp.where(part_of == c, repeated, 0.0).astype(BF16)
        copies[c].wait()
        levels += dot_dims(spectrum[c], table, 1, 1)
    spread = (iota((columns, width), 0) == iota((columns, width), 1) // slots).astype(BF16)
    expanded = dot(levels.astype(BF16), spread)
    slot_of_lane = iota((degrees, width), 1) % slots
    degree = iota((degrees, width), 0) + lax.axis_index(("half", "z")) * degrees
    first_slot = lax.axis_index(MA) * slots
    blocks = []
    for k in range(slots):
        kept = (slot_of_lane == k) & (degree >= orders[first_slot + k])
        blocks.append(jnp.where(kept, expanded[k * degrees : (k + 1) * degrees], 0.0).astype(BF16))
    diagonal = jnp.concatenate(blocks, axis=0)
    copies[parts].wait()
    total = dot_dims(legendre[...], diagonal, 0, 0).astype(BF16)
    n_z, lats, _ = out.shape
    block = lats // halves
    for h in range(halves):
        for z in range(n_z):
            at_lat = (h * n_z + z) * block
            out[z, h * block : (h + 1) * block] = total[at_lat : at_lat + block]


def table_kernel(orders, cosines, sines):
    count = orders.shape[1]
    order = jnp.broadcast_to(as_column(orders[...], count), (count, LANES))
    angle = (order * iota((count, LANES), 1) % NPHI).astype(F32) * (2.0 * math.pi / NPHI)
    weight = jnp.where(order == 0, 1.0, 2.0).astype(F32) / math.sqrt(NS)
    cosine, sine = jnp.cos(angle) * weight, jnp.sin(angle) * weight
    half_root = math.sqrt(0.5)
    for j in range(NPHI // LANES):
        eighth = order * j % 8
        size = jnp.where(eighth % 2 == 1, half_root, 1.0)
        turn_cos = jnp.where(eighth % 4 == 2, 0.0, jnp.where((eighth >= 3) & (eighth <= 5), -size, size))
        turn_sin = jnp.where(eighth % 4 == 0, 0.0, jnp.where(eighth > 4, -size, size))
        at = slice(j * LANES, (j + 1) * LANES)
        cosines[:, at] = (cosine * turn_cos - sine * turn_sin).astype(BF16)
        sines[:, at] = (-sine * turn_cos - cosine * turn_sin).astype(BF16)


def column_kernel(arrived, infos, copies, stacked):
    lats = arrived.shape[1]
    levels_n = infos.shape[1] // 2
    width = arrived.shape[2] // levels_n
    total = arrived[0].astype(F32)
    for d in range(1, arrived.shape[0]):
        total += arrived[d].astype(F32)
    points = jnp.concatenate(
        [total[:, r * width : (r + 1) * width] for r in range(levels_n)], axis=0
    ).astype(BF16)
    stacked[...] = jnp.concatenate([jnp.zeros_like(points), points], axis=1)
    half = width // 2
    exact = points.astype(F32)
    buoyancy = exact[:, :half] - COMPOSITION_WEIGHT * exact[:, half:]
    info = in_place(infos[...])
    rows = jnp.concatenate([info[:, r : r + 1] for r in range(levels_n)], axis=0)
    weight = jnp.concatenate([info[:, r : r + 1] for r in range(levels_n, 2 * levels_n)], axis=0)
    weighted = buoyancy * weight
    high = weighted.astype(BF16)
    low = (weighted - high.astype(F32)).astype(BF16)
    onehot = matches(rows, iota((lats * levels_n, NS), 1).astype(F32))
    both = dot_dims(jnp.concatenate([high, low], axis=1), onehot, 0, 0)
    column = (both[:half] + both[half:]).astype(BF16)
    copies[...] = jnp.broadcast_to(column[None], copies.shape)


def message_kernel(per, stacked, infos, base, picks):
    lats = base.shape[0] // per
    levels_n = infos.shape[1] // 2
    info = in_place(infos[...])
    q = iota((per, info.shape[1]), 0)
    own_level = (q == iota(q.shape, 1)) & (q < levels_n)
    wanted = [
        jnp.sum(jnp.where(own_level, info[t : t + 1], 0.0), axis=1, keepdims=True)
        for t in range(lats)
    ]
    absent = iota((lats * per, 1), 0) % per >= levels_n
    row = jnp.where(absent, -1.0, jnp.concatenate(wanted, axis=0))
    picks[...] = matches(row, iota((lats * per, NS), 1).astype(F32))
    count = stacked.shape[0]
    point = iota((1, count), 1)
    code = point % lats * per + point // lats
    base[...] = dot(matches(iota((lats * per, count), 0), code), stacked[...]).astype(BF16)


def select_kernel(levels_n, parts, step, picks, base, out):
    column = parts[0].astype(F32)
    for d in range(1, parts.shape[0]):
        column += parts[d].astype(F32)
    half = column.shape[0] // 2
    outward = step[...] * jnp.concatenate([column[half:], column[:half]], axis=0)
    at = iota(column.shape, 1)
    after = jnp.where(at == NS - 1, 0.0, pltpu.roll(column, NS - 1, axis=1))
    before = jnp.where(at == 0, 0.0, pltpu.roll(column, 1, axis=1))
    around = after - before
    zeros = jnp.zeros_like(column)
    points = jnp.concatenate([outward, around, zeros, zeros], axis=0).astype(BF16)
    group = at // 4 % 4
    rows = jnp.concatenate([jnp.where(group == g, column, 0.0) for g in range(4)], axis=0)
    per = out.shape[1]
    own = per - levels_n
    count = picks.shape[0]
    s = iota((1, NS), 1)
    n_ma = NS // per
    message = iota((count, 1), 0)
    q = message % per
    code = jnp.where(q >= levels_n, message // per % n_ma * own + q - levels_n, -1)
    chosen = dot_dims(picks[...], points, 1, 1)
    chosen += dot_dims(matches(code, s // per * own + s % own), rows.astype(BF16), 1, 1)
    chosen += base[...].astype(F32)
    out[...] = chosen.astype(BF16).reshape(out.shape)


def advect_kernel(levels_n, slots, got, cosines, sines, slope, radius, owned, advected):
    n_ma, per, _ = got.shape[1:]
    taken = [(got[0, b].astype(F32) + got[1, b].astype(F32)).astype(BF16) for b in range(n_ma)]
    by_part = []
    for i in range(2):
        groups = []
        for g in range(4):
            at = (2 * g + i) * slots
            groups.append(jnp.concatenate([x[:, at : at + slots] for x in taken], axis=1))
        by_part.append(groups)
    scale = slope[...]
    sides = []
    for i in range(2):
        turned = [
            (by_part[1 - i][g].astype(F32) * (scale if i else -scale)).astype(BF16) for g in (2, 3)
        ]
        sides.append(jnp.concatenate(by_part[i] + turned, axis=0))
    result = dot(sides[0], cosines[...]) + dot(sides[1], sines[...])
    rows = [result[g * per : g * per + levels_n] for g in range(6)]
    inverse = 1.0 / radius[...]
    outward = rows[0] * (0.5 * inverse)
    around = -0.5 * rows[1]
    held = [x.astype(BF16).astype(F32) for x in rows[2:]]
    for f in range(2):
        field, side = held[f], held[2 + f]
        value = field - (TIME_STEP * inverse) * (around * side + outward * field)
        for r in range(levels_n):
            advected[f, r] = value[r : r + 1]
    mine = jnp.concatenate([result[g * per + levels_n : (g + 1) * per] for g in range(4)], axis=0)
    width = owned.shape[1]
    start = lax.axis_index(("half", "z")) * width
    mine = pltpu.roll(mine, lax.rem(NPHI - start, NPHI), axis=1)
    owned[...] = mine[:, :width]


def in_hbm(array):
    return pltpu.with_memory_space_constraint(array, pltpu.HBM)


def exchanged(blocks, axis):
    return lax.all_to_all(blocks, axis, split_axis=0, concat_axis=0, tiled=True)


def on_device(spectrum, radial_table, legendre, order_table, cylinder_row, column_weight):
    parts, slots, degrees, modes = spectrum.shape
    levels_n = radial_table.shape[0]
    lats = legendre.shape[2]
    n_z = lax.axis_size("z")
    n_half = lax.axis_size("half")
    n_ma = lax.axis_size(MA)
    lat_block = lats // n_z
    row_block = NS // n_ma
    lon_block = NPHI // (n_half * n_z)
    me_ma = lax.axis_index(MA)
    swap = [(0, 1), (1, 0)]

    near = ("y", "x", "core")
    info = vmem_call(
        info_kernel,
        pltpu.HBM((lax.axis_size(near), 1, 2 * levels_n), F32),
        0, 2,
    )(in_hbm(cylinder_row), in_hbm(column_weight))
    info = exchanged(info, near).reshape(-1, 2 * levels_n)
    contribution = vmem_call(
        functools.partial(contribution_kernel, slots, degrees, n_half),
        pltpu.HBM((n_z, lat_block, levels_n * parts * slots), BF16),
        1, 1, 2,
        (
            pltpu.VMEM((parts, slots * degrees, modes), BF16),
            pltpu.VMEM((slots * degrees, lats), BF16),
            pltpu.SemaphoreType.DMA((parts + 1,)),
        ),
    )(
        in_hbm(order_table),
        in_hbm(radial_table),
        in_hbm(spectrum.reshape(parts, slots * degrees, modes)),
        in_hbm(legendre.reshape(slots * degrees, lats)),
    )
    arrived = exchanged(contribution, "z")
    info = jnp.concatenate([info, lax.ppermute(info, "pair", swap)], axis=0)
    infos = jnp.concatenate([info, lax.ppermute(info, "half", swap)], axis=0)
    my_orders = lax.dynamic_slice_in_dim(order_table, me_ma * slots, slots)
    step = 2.0 * jnp.sin(my_orders.astype(F32) * (2.0 * math.pi / NPHI))
    step = jnp.concatenate([-step, step]).reshape(2 * slots, 1)
    slope = (order_table.astype(F32) / NS).reshape(1, -1)
    radius = (0.35 + 0.65 * (cylinder_row.astype(F32) + 0.5) / NS).reshape(levels_n, 1)
    copies, stacked = vmem_call(
        column_kernel,
        (
            pltpu.HBM((n_z, 2 * slots, NS), BF16),
            jax.ShapeDtypeStruct((levels_n * lat_block, LANES), BF16),
        ),
        0, 2,
    )(arrived, infos)
    partials = exchanged(copies, "z")
    base, picks = vmem_call(
        functools.partial(message_kernel, row_block),
        (
            jax.ShapeDtypeStruct((lat_block * row_block, LANES), BF16),
            jax.ShapeDtypeStruct((lat_block * row_block, NS), BF16),
        ),
        0, 2,
    )(stacked, infos)
    chosen = vmem_call(
        functools.partial(select_kernel, levels_n),
        pltpu.HBM((lat_block, row_block, LANES), BF16),
        0, 4,
    )(partials, step, picks, base)
    got = exchanged(chosen, ("half", *MA)).reshape(n_half, n_ma, row_block, LANES)
    table = jax.ShapeDtypeStruct((lats, NPHI), BF16)
    cosines, sines = vmem_call(table_kernel, (table, table), 0, 1)(order_table.reshape(1, -1))
    owned, advected = vmem_call(
        functools.partial(advect_kernel, levels_n, slots),
        (
            jax.ShapeDtypeStruct((row_block, lon_block), F32),
            jax.ShapeDtypeStruct((2, levels_n, 1, NPHI), F32),
        ),
        0, 5,
    )(got, cosines, sines, slope, radius)
    return (owned, jnp.swapaxes(advected, 1, 2))


def solution(mesh):
    parts = Mesh(
        mesh.devices.reshape(HALVES, -1, PAIRS, PAIRS, mesh.shape["ma"] // 8, 2),
        ("half", "z", *MA),
    )
    rad = ("half", "z")
    return jax.shard_map(
        on_device,
        mesh=parts,
        in_specs=(
            P(None, MA, rad, None),
            P(),
            P(MA, rad, None),
            P(),
            P((*rad, *MA), None),
            P((*rad, *MA), None),
        ),
        out_specs=(P(MA, rad), P(None, (*rad, *MA), None, None)),
        check_vma=False,
    )
```

```python
import functools
import math

import jax
import jax.numpy as jnp
from jax import lax
from jax.experimental import pallas as pl
from jax.experimental.pallas import tpu as pltpu
from jax.sharding import Mesh
from jax.sharding import PartitionSpec as P

NPHI = 1024
NS = 512
LANES = 128
HALVES = 2
PAIRS = 2
MA = ("pair", "y", "x", "core")
VMEM_LIMIT = 20 * 2**20
TIME_STEP = 0.05
COMPOSITION_WEIGHT = 0.8
BF16 = jnp.bfloat16
F32 = jnp.float32
I32 = jnp.int32

dot = functools.partial(jnp.dot, preferred_element_type=F32)


def iota(shape, dim):
    return lax.broadcasted_iota(I32, shape, dim)


def as_column(row, width):
    return jnp.transpose(jnp.broadcast_to(row, (8, width)))[:, :1]


def matches(column, row):
    return (column == row).astype(F32).astype(BF16)


def dot_dims(x, y, dim_x, dim_y):
    return lax.dot_general(x, y, (((dim_x,), (dim_y,)), ((), ())), preferred_element_type=F32)


def vmem_call(body, outs, n_smem, n_vmem, n_hbm=0, scratch=()):
    return pl.pallas_call(
        body,
        out_shape=outs,
        in_specs=[pl.BlockSpec(memory_space=pltpu.SMEM)] * n_smem
        + [pl.BlockSpec(memory_space=pltpu.VMEM)] * n_vmem
        + [pl.BlockSpec(memory_space=pltpu.HBM)] * n_hbm,
        out_specs=jax.tree.map(lambda _: pl.BlockSpec(memory_space=pltpu.VMEM), outs),
        scratch_shapes=scratch,
        compiler_params=pltpu.CompilerParams(vmem_limit_bytes=VMEM_LIMIT),
    )


def info_kernel(rows, weights, out):
    info = jnp.concatenate([rows[...].astype(F32), weights[...]], axis=1)
    for d in range(out.shape[0]):
        out[d] = info


def in_place(infos):
    count = infos.shape[0] // 4
    pieces = [infos[j * count : (j + 1) * count] for j in range(4)]
    pair, half = lax.axis_index("pair") == 0, lax.axis_index("half") == 0
    halves = [
        jnp.concatenate([jnp.where(pair, a, b), jnp.where(pair, b, a)], axis=0)
        for a, b in (pieces[:2], pieces[2:])
    ]
    a, b = halves
    return jnp.concatenate([jnp.where(half, a, b), jnp.where(half, b, a)], axis=0)


def contribution_kernel(
    slots, degrees, halves, orders, radial, spectrum_in, legendre_in, out, spectrum, legendre, sems
):
    parts = spectrum.shape[0]
    copies = [
        pltpu.make_async_copy(spectrum_in.at[c], spectrum.at[c], sems.at[c]) for c in range(parts)
    ]
    copies.append(pltpu.make_async_copy(legendre_in, legendre, sems.at[parts]))
    for copy in copies:
        copy.start()
    levels_n = radial.shape[0]
    columns = levels_n * parts
    width = columns * slots
    rows = slots * degrees
    repeat = (iota((columns, levels_n), 0) // parts == iota((columns, levels_n), 1)).astype(BF16)
    repeated = dot(repeat, radial[...])
    part_of = iota(repeated.shape, 0) % parts
    levels = jnp.zeros((rows, columns), F32)
    for c in range(parts):
        table = jnp.where(part_of == c, repeated, 0.0).astype(BF16)
        copies[c].wait()
        levels += dot_dims(spectrum[c], table, 1, 1)
    spread = (iota((columns, width), 0) == iota((columns, width), 1) // slots).astype(BF16)
    expanded = dot(levels.astype(BF16), spread)
    slot_of_lane = iota((degrees, width), 1) % slots
    degree = iota((degrees, width), 0) + lax.axis_index(("half", "z")) * degrees
    first_slot = lax.axis_index(MA) * slots
    blocks = []
    for k in range(slots):
        kept = (slot_of_lane == k) & (degree >= orders[first_slot + k])
        blocks.append(jnp.where(kept, expanded[k * degrees : (k + 1) * degrees], 0.0).astype(BF16))
    diagonal = jnp.concatenate(blocks, axis=0)
    copies[parts].wait()
    total = dot_dims(legendre[...], diagonal, 0, 0).astype(BF16)
    n_z, lats, _ = out.shape
    block = lats // halves
    for h in range(halves):
        for z in range(n_z):
            at_lat = (h * n_z + z) * block
            out[z, h * block : (h + 1) * block] = total[at_lat : at_lat + block]


def table_kernel(orders, cosines, sines):
    count = orders.shape[1]
    order = jnp.broadcast_to(as_column(orders[...], count), (count, LANES))
    angle = (order * iota((count, LANES), 1) % NPHI).astype(F32) * (2.0 * math.pi / NPHI)
    weight = jnp.where(order == 0, 1.0, 2.0).astype(F32) / math.sqrt(NS)
    cosine, sine = jnp.cos(angle) * weight, jnp.sin(angle) * weight
    half_root = math.sqrt(0.5)
    for j in range(NPHI // LANES):
        eighth = order * j % 8
        size = jnp.where(eighth % 2 == 1, half_root, 1.0)
        turn_cos = jnp.where(eighth % 4 == 2, 0.0, jnp.where((eighth >= 3) & (eighth <= 5), -size, size))
        turn_sin = jnp.where(eighth % 4 == 0, 0.0, jnp.where(eighth > 4, -size, size))
        at = slice(j * LANES, (j + 1) * LANES)
        cosines[:, at] = (cosine * turn_cos - sine * turn_sin).astype(BF16)
        sines[:, at] = (-sine * turn_cos - cosine * turn_sin).astype(BF16)


def choice_kernel(per, infos, picks):
    lats = infos.shape[0]
    levels_n = infos.shape[1] // 2
    info = in_place(infos[...])
    q = iota((per, info.shape[1]), 0)
    own_level = (q == iota(q.shape, 1)) & (q < levels_n)
    wanted = [
        jnp.sum(jnp.where(own_level, info[t : t + 1], 0.0), axis=1, keepdims=True)
        for t in range(lats)
    ]
    absent = iota((lats * per, 1), 0) % per >= levels_n
    row = jnp.where(absent, -1.0, jnp.concatenate(wanted, axis=0))
    picks[...] = matches(row, iota(picks.shape, 1).astype(F32))


def column_kernel(per, arrived, infos, copies, base):
    lats = arrived.shape[1]
    levels_n = infos.shape[1] // 2
    width = arrived.shape[2] // levels_n
    total = arrived[0].astype(F32)
    for d in range(1, arrived.shape[0]):
        total += arrived[d].astype(F32)
    points = jnp.concatenate(
        [total[:, r * width : (r + 1) * width] for r in range(levels_n)], axis=0
    ).astype(BF16)
    info = in_place(infos[...])
    rows = jnp.concatenate([info[:, r : r + 1] for r in range(levels_n)], axis=0)
    weight = jnp.concatenate([info[:, r : r + 1] for r in range(levels_n, 2 * levels_n)], axis=0)
    onehot = matches(rows, iota((lats * levels_n, NS), 1).astype(F32))
    half = width // 2
    exact = points.astype(F32)
    weighted = (exact[:, :half] - COMPOSITION_WEIGHT * exact[:, half:]) * weight
    high = weighted.astype(BF16)
    low = (weighted - high.astype(F32)).astype(BF16)
    both = dot_dims(jnp.concatenate([high, low], axis=1), onehot, 0, 0)
    column = (both[:half] + both[half:]).astype(BF16)
    copies[...] = jnp.broadcast_to(column[None], copies.shape)
    stacked = jnp.concatenate([jnp.zeros_like(points), points], axis=1)
    point = iota((1, lats * levels_n), 1)
    places = matches(iota((lats * per, 1), 0), point % lats * per + point // lats)
    base[...] = dot(places, stacked).astype(BF16)


def select_kernel(levels_n, parts, step, picks, base, out):
    column = parts[0].astype(F32)
    for d in range(1, parts.shape[0]):
        column += parts[d].astype(F32)
    half = column.shape[0] // 2
    outward = as_column(step[...], step.shape[1]) * jnp.concatenate(
        [column[half:], column[:half]], axis=0
    )
    at = iota(column.shape, 1)
    after = jnp.where(at == NS - 1, 0.0, pltpu.roll(column, NS - 1, axis=1))
    before = jnp.where(at == 0, 0.0, pltpu.roll(column, 1, axis=1))
    around = after - before
    zeros = jnp.zeros_like(column)
    points = jnp.concatenate([outward, around, zeros, zeros], axis=0).astype(BF16)
    group = at // 4 % 4
    rows = jnp.concatenate([jnp.where(group == g, column, 0.0) for g in range(4)], axis=0)
    chosen = dot_dims(picks[...], points, 1, 1)
    per = out.shape[1]
    own = per - levels_n
    message = iota((picks.shape[0], 1), 0)
    level = message % per
    code = jnp.where(level >= levels_n, message // per % (NS // per) * own + level - levels_n, -1)
    s = iota((1, NS), 1)
    chosen += dot_dims(matches(code, s // per * own + s % own), rows.astype(BF16), 1, 1)
    chosen += base[...].astype(F32)
    out[...] = chosen.astype(BF16).reshape(out.shape)


def advect_kernel(levels_n, slots, got, cosines, sines, slope, radius, owned, advected):
    n_ma, per, _ = got.shape[1:]
    taken = [(got[0, b].astype(F32) + got[1, b].astype(F32)).astype(BF16) for b in range(n_ma)]
    by_part = []
    for i in range(2):
        groups = []
        for g in range(4):
            at = (2 * g + i) * slots
            groups.append(jnp.concatenate([x[:, at : at + slots] for x in taken], axis=1))
        by_part.append(groups)
    scale = slope[...]
    sides = []
    for i in range(2):
        turned = [
            (by_part[1 - i][g].astype(F32) * (scale if i else -scale)).astype(BF16) for g in (2, 3)
        ]
        sides.append(jnp.concatenate(by_part[i] + turned, axis=0))
    result = dot(sides[0], cosines[...]) + dot(sides[1], sines[...])
    rows = [result[g * per : g * per + levels_n] for g in range(6)]
    inverse = 1.0 / as_column(radius[...], levels_n)
    outward = rows[0] * (0.5 * inverse)
    around = -0.5 * rows[1]
    held = [x.astype(BF16).astype(F32) for x in rows[2:]]
    for f in range(2):
        field, side = held[f], held[2 + f]
        value = field - (TIME_STEP * inverse) * (around * side + outward * field)
        for r in range(levels_n):
            advected[f, r] = value[r : r + 1]
    mine = jnp.concatenate([result[g * per + levels_n : (g + 1) * per] for g in range(4)], axis=0)
    width = owned.shape[1]
    start = lax.axis_index(("half", "z")) * width
    mine = pltpu.roll(mine, lax.rem(NPHI - start, NPHI), axis=1)
    owned[...] = mine[:, :width]


def in_hbm(array):
    return pltpu.with_memory_space_constraint(array, pltpu.HBM)


def exchanged(blocks, axis):
    return lax.all_to_all(blocks, axis, split_axis=0, concat_axis=0, tiled=True)


def on_device(spectrum, radial_table, legendre, order_table, cylinder_row, column_weight):
    parts, slots, degrees, modes = spectrum.shape
    levels_n = radial_table.shape[0]
    lats = legendre.shape[2]
    n_z = lax.axis_size("z")
    n_half = lax.axis_size("half")
    n_ma = lax.axis_size(MA)
    lat_block = lats // n_z
    row_block = NS // n_ma
    lon_block = NPHI // (n_half * n_z)
    me_ma = lax.axis_index(MA)
    swap = [(0, 1), (1, 0)]

    near = ("y", "x", "core")
    info = vmem_call(
        info_kernel,
        pltpu.HBM((lax.axis_size(near), 1, 2 * levels_n), F32),
        0, 2,
    )(in_hbm(cylinder_row), in_hbm(column_weight))
    info = exchanged(info, near).reshape(-1, 2 * levels_n)
    contribution = vmem_call(
        functools.partial(contribution_kernel, slots, degrees, n_half),
        pltpu.HBM((n_z, lat_block, levels_n * parts * slots), BF16),
        1, 1, 2,
        (
            pltpu.VMEM((parts, slots * degrees, modes), BF16),
            pltpu.VMEM((slots * degrees, lats), BF16),
            pltpu.SemaphoreType.DMA((parts + 1,)),
        ),
    )(
        in_hbm(order_table),
        in_hbm(radial_table),
        in_hbm(spectrum.reshape(parts, slots * degrees, modes)),
        in_hbm(legendre.reshape(slots * degrees, lats)),
    )
    arrived = exchanged(contribution, "z")
    info = jnp.concatenate([info, lax.ppermute(info, "pair", swap)], axis=0)
    infos = jnp.concatenate([info, lax.ppermute(info, "half", swap)], axis=0)
    my_orders = lax.dynamic_slice_in_dim(order_table, me_ma * slots, slots)
    step = 2.0 * jnp.sin(my_orders.astype(F32) * (2.0 * math.pi / NPHI))
    step = jnp.concatenate([-step, step]).reshape(1, -1)
    slope = (order_table.astype(F32) / NS).reshape(1, -1)
    radius = (0.35 + 0.65 * (cylinder_row.astype(F32) + 0.5) / NS).reshape(1, -1)
    table = jax.ShapeDtypeStruct((lats, NPHI), BF16)
    cosines, sines = vmem_call(table_kernel, (table, table), 0, 1)(order_table.reshape(1, -1))
    messages = lat_block * row_block
    picks = vmem_call(
        functools.partial(choice_kernel, row_block),
        jax.ShapeDtypeStruct((messages, NS), BF16),
        0, 1,
    )(infos)
    arrived, cosines, sines, step, slope, radius, infos, picks = lax.optimization_barrier(
        (arrived, cosines, sines, step, slope, radius, infos, picks)
    )
    copies, base = vmem_call(
        functools.partial(column_kernel, row_block),
        (
            jax.ShapeDtypeStruct((n_z, 2 * slots, NS), BF16),
            jax.ShapeDtypeStruct((messages, LANES), BF16),
        ),
        0, 2,
    )(arrived, infos)
    partials = exchanged(copies, "z")
    chosen = vmem_call(
        functools.partial(select_kernel, levels_n),
        jax.ShapeDtypeStruct((lat_block, row_block, LANES), BF16),
        0, 4,
    )(partials, step, picks, base)
    got = exchanged(chosen, ("half", *MA)).reshape(n_half, n_ma, row_block, LANES)
    owned, advected = vmem_call(
        functools.partial(advect_kernel, levels_n, slots),
        (
            jax.ShapeDtypeStruct((row_block, lon_block), F32),
            jax.ShapeDtypeStruct((2, levels_n, 1, NPHI), F32),
        ),
        0, 5,
    )(got, cosines, sines, slope, radius)
    return (owned, jnp.swapaxes(advected, 1, 2))


def solution(mesh):
    parts = Mesh(
        mesh.devices.reshape(HALVES, -1, PAIRS, PAIRS, mesh.shape["ma"] // 8, 2),
        ("half", "z", *MA),
    )
    rad = ("half", "z")
    return jax.shard_map(
        on_device,
        mesh=parts,
        in_specs=(
            P(None, MA, rad, None),
            P(),
            P(MA, rad, None),
            P(),
            P((*rad, *MA), None),
            P((*rad, *MA), None),
        ),
        out_specs=(P(MA, rad), P(None, (*rad, *MA), None, None)),
        check_vma=False,
    )
```

```python
import functools
import math

import jax
import jax.numpy as jnp
from jax import lax
from jax.experimental import pallas as pl
from jax.experimental.pallas import tpu as pltpu
from jax.sharding import Mesh
from jax.sharding import PartitionSpec as P

NPHI = 1024
NS = 512
LANES = 128
HALVES = 2
PAIRS = 2
MA = ("pair", "y", "x", "core")
VMEM_LIMIT = 20 * 2**20
TIME_STEP = 0.05
COMPOSITION_WEIGHT = 0.8
BF16 = jnp.bfloat16
F32 = jnp.float32
I32 = jnp.int32

dot = functools.partial(jnp.dot, preferred_element_type=F32)


def iota(shape, dim):
    return lax.broadcasted_iota(I32, shape, dim)


def as_column(row, width):
    return jnp.transpose(jnp.broadcast_to(row, (8, width)))[:, :1]


def matches(column, row):
    return (column == row).astype(F32).astype(BF16)


def dot_dims(x, y, dim_x, dim_y):
    return lax.dot_general(x, y, (((dim_x,), (dim_y,)), ((), ())), preferred_element_type=F32)


def vmem_call(body, outs, n_smem, n_vmem, n_hbm=0, scratch=(), out_space=pltpu.VMEM):
    return pl.pallas_call(
        body,
        out_shape=outs,
        in_specs=[pl.BlockSpec(memory_space=pltpu.SMEM)] * n_smem
        + [pl.BlockSpec(memory_space=pltpu.VMEM)] * n_vmem
        + [pl.BlockSpec(memory_space=pltpu.HBM)] * n_hbm,
        out_specs=jax.tree.map(lambda _: pl.BlockSpec(memory_space=out_space), outs),
        scratch_shapes=scratch,
        compiler_params=pltpu.CompilerParams(vmem_limit_bytes=VMEM_LIMIT),
    )


def info_kernel(rows, weights, out):
    info = jnp.concatenate([rows[...].astype(F32), weights[...]], axis=1)
    for d in range(out.shape[0]):
        out[d] = info


def in_place(infos):
    count = infos.shape[0] // 4
    pieces = [infos[j * count : (j + 1) * count] for j in range(4)]
    pair, half = lax.axis_index("pair") == 0, lax.axis_index("half") == 0
    halves = [
        jnp.concatenate([jnp.where(pair, a, b), jnp.where(pair, b, a)], axis=0)
        for a, b in (pieces[:2], pieces[2:])
    ]
    a, b = halves
    return jnp.concatenate([jnp.where(half, a, b), jnp.where(half, b, a)], axis=0)


def contribution_kernel(
    slots, degrees, halves, orders, radial, spectrum_in, legendre_in, out,
    spectrum, legendre, turned, held, sems, outs
):
    parts = spectrum.shape[0]
    ways = sems.shape[1]
    step = spectrum.shape[1] // ways
    sides = [(legendre_in, legendre)] + [(spectrum_in.at[c], spectrum.at[c]) for c in range(parts)]
    copies = [
        [
            pltpu.make_async_copy(
                source.at[pl.ds(w * step, step)], target.at[pl.ds(w * step, step)], sems.at[c, w]
            )
            for w in range(ways)
        ]
        for c, (source, target) in enumerate(sides)
    ]
    for some in copies:
        for copy in some:
            copy.start()
    for copy in copies[0]:
        copy.wait()
    turned[...] = jnp.transpose(legendre[...])
    levels_n = radial.shape[0]
    columns = levels_n * parts
    width = columns * slots
    rows = slots * degrees
    repeat = (iota((columns, levels_n), 0) // parts == iota((columns, levels_n), 1)).astype(BF16)
    repeated = dot(repeat, radial[...])
    part_of = iota(repeated.shape, 0) % parts
    levels = jnp.zeros((rows, columns), F32)
    for c in range(parts):
        table = jnp.where(part_of == c, repeated, 0.0).astype(BF16)
        for copy in copies[c + 1]:
            copy.wait()
        levels += dot_dims(spectrum[c], table, 1, 1)
    spread = (iota((columns, width), 0) == iota((columns, width), 1) // slots).astype(BF16)
    expanded = dot(levels.astype(BF16), spread)
    slot_of_lane = iota((degrees, width), 1) % slots
    degree = iota((degrees, width), 0) + lax.axis_index(("half", "z")) * degrees
    first_slot = lax.axis_index(MA) * slots
    blocks = []
    for k in range(slots):
        kept = (slot_of_lane == k) & (degree >= orders[first_slot + k])
        blocks.append(jnp.where(kept, expanded[k * degrees : (k + 1) * degrees], 0.0).astype(BF16))
    diagonal = jnp.concatenate(blocks, axis=0)
    n_z, lats, _ = out.shape
    block = lats // halves
    group = LANES // block
    writes = []
    for first in range(0, halves * n_z, group):
        lanes = slice(first * block, (first + group) * block)
        held[lanes] = dot(turned[lanes], diagonal).astype(BF16)
        for g in range(first, first + group):
            h, z = divmod(g, n_z)
            write = pltpu.make_async_copy(
                held.at[pl.ds(g * block, block)], out.at[z, pl.ds(h * block, block)], outs.at[g]
            )
            write.start()
            writes.append(write)
    for write in writes:
        write.wait()


def table_kernel(orders, cosines, sines):
    count = orders.shape[1]
    order = jnp.broadcast_to(as_column(orders[...], count), (count, LANES))
    angle = (order * iota((count, LANES), 1) & (NPHI - 1)).astype(F32) * (2.0 * math.pi / NPHI)
    weight = jnp.where(order == 0, 1.0, 2.0).astype(F32) / math.sqrt(NS)
    cosine, sine = jnp.cos(angle) * weight, jnp.sin(angle) * weight
    half_root = math.sqrt(0.5)
    for j in range(NPHI // LANES):
        eighth = order * j & 7
        size = jnp.where(eighth & 1 == 1, half_root, 1.0)
        turn_cos = jnp.where(eighth & 3 == 2, 0.0, jnp.where((eighth >= 3) & (eighth <= 5), -size, size))
        turn_sin = jnp.where(eighth & 3 == 0, 0.0, jnp.where(eighth > 4, -size, size))
        at = slice(j * LANES, (j + 1) * LANES)
        cosines[:, at] = (cosine * turn_cos - sine * turn_sin).astype(BF16)
        sines[:, at] = (-sine * turn_cos - cosine * turn_sin).astype(BF16)


def choice_kernel(per, infos, picks):
    lats = infos.shape[0]
    levels_n = infos.shape[1] // 2
    info = in_place(infos[...])
    q = iota((per, info.shape[1]), 0)
    own_level = (q == iota(q.shape, 1)) & (q < levels_n)
    wanted = [
        jnp.sum(jnp.where(own_level, info[t : t + 1], 0.0), axis=1, keepdims=True)
        for t in range(lats)
    ]
    absent = iota((lats * per, 1), 0) % per >= levels_n
    row = jnp.where(absent, -1.0, jnp.concatenate(wanted, axis=0))
    picks[...] = matches(row, iota(picks.shape, 1).astype(F32))


def column_kernel(per, arrived, infos, copies, base):
    lats = arrived.shape[1]
    levels_n = infos.shape[1] // 2
    width = arrived.shape[2] // levels_n
    total = arrived[0].astype(F32)
    for d in range(1, arrived.shape[0]):
        total += arrived[d].astype(F32)
    points = jnp.concatenate(
        [total[:, r * width : (r + 1) * width] for r in range(levels_n)], axis=0
    ).astype(BF16)
    info = in_place(infos[...])
    rows = jnp.concatenate([info[:, r : r + 1] for r in range(levels_n)], axis=0)
    weight = jnp.concatenate([info[:, r : r + 1] for r in range(levels_n, 2 * levels_n)], axis=0)
    onehot = matches(rows, iota((lats * levels_n, NS), 1).astype(F32))
    half = width // 2
    exact = points.astype(F32)
    weighted = (exact[:, :half] - COMPOSITION_WEIGHT * exact[:, half:]) * weight
    high = weighted.astype(BF16)
    low = (weighted - high.astype(F32)).astype(BF16)
    both = dot_dims(jnp.concatenate([high, low], axis=1), onehot, 0, 0)
    column = (both[:half] + both[half:]).astype(BF16)
    copies[...] = jnp.broadcast_to(column[None], copies.shape)
    stacked = jnp.concatenate([jnp.zeros_like(points), points], axis=1)
    point = iota((1, lats * levels_n), 1)
    places = matches(iota((lats * per, 1), 0), point % lats * per + point // lats)
    base[...] = dot(places, stacked).astype(BF16)


def select_kernel(levels_n, parts, step, picks, base, out):
    column = parts[0].astype(F32)
    for d in range(1, parts.shape[0]):
        column += parts[d].astype(F32)
    half = column.shape[0] // 2
    outward = as_column(step[...], step.shape[1]) * jnp.concatenate(
        [column[half:], column[:half]], axis=0
    )
    at = iota(column.shape, 1)
    after = jnp.where(at == NS - 1, 0.0, pltpu.roll(column, NS - 1, axis=1))
    before = jnp.where(at == 0, 0.0, pltpu.roll(column, 1, axis=1))
    around = after - before
    zeros = jnp.zeros_like(column)
    points = jnp.concatenate([outward, around, zeros, zeros], axis=0).astype(BF16)
    group = at // 4 % 4
    rows = jnp.concatenate([jnp.where(group == g, column, 0.0) for g in range(4)], axis=0)
    chosen = dot_dims(picks[...], points, 1, 1)
    per = out.shape[1]
    own = per - levels_n
    message = iota((picks.shape[0], 1), 0)
    level = message % per
    code = jnp.where(level >= levels_n, message // per % (NS // per) * own + level - levels_n, -1)
    s = iota((1, NS), 1)
    chosen += dot_dims(matches(code, s // per * own + s % own), rows.astype(BF16), 1, 1)
    chosen += base[...].astype(F32)
    out[...] = chosen.astype(BF16).reshape(out.shape)


def advect_kernel(levels_n, slots, got, cosines, sines, slope, radius, owned, advected):
    n_ma, per, _ = got.shape[1:]
    taken = [(got[0, b].astype(F32) + got[1, b].astype(F32)).astype(BF16) for b in range(n_ma)]
    by_part = []
    for i in range(2):
        groups = []
        for g in range(4):
            at = (2 * g + i) * slots
            groups.append(jnp.concatenate([x[:, at : at + slots] for x in taken], axis=1))
        by_part.append(groups)
    scale = slope[...]
    sides = []
    for i in range(2):
        turned = [
            (by_part[1 - i][g].astype(F32) * (scale if i else -scale)).astype(BF16) for g in (2, 3)
        ]
        sides.append(jnp.concatenate(by_part[i] + turned, axis=0))
    result = dot(sides[0], cosines[...]) + dot(sides[1], sines[...])
    rows = [result[g * per : g * per + levels_n] for g in range(6)]
    inverse = 1.0 / as_column(radius[...], levels_n)
    outward = rows[0] * (0.5 * inverse)
    around = -0.5 * rows[1]
    held = [x.astype(BF16).astype(F32) for x in rows[2:]]
    for f in range(2):
        field, side = held[f], held[2 + f]
        value = field - (TIME_STEP * inverse) * (around * side + outward * field)
        for r in range(levels_n):
            advected[f, r] = value[r : r + 1]
    mine = jnp.concatenate([result[g * per + levels_n : (g + 1) * per] for g in range(4)], axis=0)
    width = owned.shape[1]
    start = lax.axis_index(("half", "z")) * width
    mine = pltpu.roll(mine, lax.rem(NPHI - start, NPHI), axis=1)
    owned[...] = mine[:, :width]


def in_hbm(array):
    return pltpu.with_memory_space_constraint(array, pltpu.HBM)


def exchanged(blocks, axis):
    return lax.all_to_all(blocks, axis, split_axis=0, concat_axis=0, tiled=True)


def on_device(spectrum, radial_table, legendre, order_table, cylinder_row, column_weight):
    parts, slots, degrees, modes = spectrum.shape
    levels_n = radial_table.shape[0]
    lats = legendre.shape[2]
    n_z = lax.axis_size("z")
    n_half = lax.axis_size("half")
    n_ma = lax.axis_size(MA)
    lat_block = lats // n_z
    row_block = NS // n_ma
    lon_block = NPHI // (n_half * n_z)
    me_ma = lax.axis_index(MA)
    swap = [(0, 1), (1, 0)]

    near = ("y", "x")
    info = vmem_call(
        info_kernel,
        pltpu.HBM((lax.axis_size(near), 1, 2 * levels_n), F32),
        0, 2,
    )(in_hbm(cylinder_row), in_hbm(column_weight))
    info = exchanged(info, near).reshape(-1, 2 * levels_n)
    contribution = vmem_call(
        functools.partial(contribution_kernel, slots, degrees, n_half),
        pltpu.HBM((n_z, lat_block, levels_n * parts * slots), BF16),
        1, 1, 2,
        (
            pltpu.VMEM((parts, slots * degrees, modes), BF16),
            pltpu.VMEM((slots * degrees, lats), BF16),
            pltpu.VMEM((lats, slots * degrees), BF16),
            pltpu.VMEM((lats, levels_n * parts * slots), BF16),
            pltpu.SemaphoreType.DMA((parts + 1, 4)),
            pltpu.SemaphoreType.DMA((n_half * n_z,)),
        ),
        pltpu.HBM,
    )(
        in_hbm(order_table),
        in_hbm(radial_table),
        in_hbm(spectrum.reshape(parts, slots * degrees, modes)),
        in_hbm(legendre.reshape(slots * degrees, lats)),
    )
    arrived = exchanged(contribution, "z")
    info = lax.all_gather(info, "core", axis=1).reshape(-1, 2 * levels_n)
    info = jnp.concatenate([info, lax.ppermute(info, "pair", swap)], axis=0)
    infos = jnp.concatenate([info, lax.ppermute(info, "half", swap)], axis=0)
    my_orders = lax.dynamic_slice_in_dim(order_table, me_ma * slots, slots)
    step = 2.0 * jnp.sin(my_orders.astype(F32) * (2.0 * math.pi / NPHI))
    step = jnp.concatenate([-step, step]).reshape(1, -1)
    slope = (order_table.astype(F32) / NS).reshape(1, -1)
    radius = (0.35 + 0.65 * (cylinder_row.astype(F32) + 0.5) / NS).reshape(1, -1)
    table = jax.ShapeDtypeStruct((lats, NPHI), BF16)
    cosines, sines = vmem_call(table_kernel, (table, table), 0, 1)(order_table.reshape(1, -1))
    messages = lat_block * row_block
    picks = vmem_call(
        functools.partial(choice_kernel, row_block),
        jax.ShapeDtypeStruct((messages, NS), BF16),
        0, 1,
    )(infos)
    arrived, cosines, sines, step, slope, radius, infos, picks = lax.optimization_barrier(
        (arrived, cosines, sines, step, slope, radius, infos, picks)
    )
    copies, base = vmem_call(
        functools.partial(column_kernel, row_block),
        (
            jax.ShapeDtypeStruct((n_z, 2 * slots, NS), BF16),
            jax.ShapeDtypeStruct((messages, LANES), BF16),
        ),
        0, 2,
    )(arrived, infos)
    partials = exchanged(copies, "z")
    chosen = vmem_call(
        functools.partial(select_kernel, levels_n),
        jax.ShapeDtypeStruct((lat_block, row_block, LANES), BF16),
        0, 4,
    )(partials, step, picks, base)
    got = exchanged(chosen, ("half", *MA)).reshape(n_half, n_ma, row_block, LANES)
    owned, advected = vmem_call(
        functools.partial(advect_kernel, levels_n, slots),
        (
            jax.ShapeDtypeStruct((row_block, lon_block), F32),
            jax.ShapeDtypeStruct((2, levels_n, 1, NPHI), F32),
        ),
        0, 5,
    )(got, cosines, sines, slope, radius)
    return (owned, jnp.swapaxes(advected, 1, 2))


def solution(mesh):
    parts = Mesh(
        mesh.devices.reshape(HALVES, -1, PAIRS, PAIRS, mesh.shape["ma"] // 8, 2),
        ("half", "z", *MA),
    )
    rad = ("half", "z")
    return jax.shard_map(
        on_device,
        mesh=parts,
        in_specs=(
            P(None, MA, rad, None),
            P(),
            P(MA, rad, None),
            P(),
            P((*rad, *MA), None),
            P((*rad, *MA), None),
        ),
        out_specs=(P(MA, rad), P(None, (*rad, *MA), None, None)),
        check_vma=False,
    )
```

```python
import functools
import math

import jax
import jax.numpy as jnp
from jax import lax
from jax.experimental import pallas as pl
from jax.experimental.pallas import tpu as pltpu
from jax.sharding import Mesh
from jax.sharding import PartitionSpec as P

NPHI = 1024
NS = 512
LANES = 128
HALVES = 2
PAIRS = 2
MA = ("pair", "y", "x", "core")
VMEM_LIMIT = 20 * 2**20
TIME_STEP = 0.05
COMPOSITION_WEIGHT = 0.8
BF16 = jnp.bfloat16
F32 = jnp.float32
I32 = jnp.int32

dot = functools.partial(jnp.dot, preferred_element_type=F32)


def iota(shape, dim):
    return lax.broadcasted_iota(I32, shape, dim)


def as_column(row, width):
    return jnp.transpose(jnp.broadcast_to(row, (8, width)))[:, :1]


def matches(column, row):
    return (column == row).astype(F32).astype(BF16)


def dot_dims(x, y, dim_x, dim_y):
    return lax.dot_general(x, y, (((dim_x,), (dim_y,)), ((), ())), preferred_element_type=F32)


def vmem_call(body, outs, n_smem, n_vmem, n_hbm=0, scratch=(), out_space=pltpu.VMEM):
    return pl.pallas_call(
        body,
        out_shape=outs,
        in_specs=[pl.BlockSpec(memory_space=pltpu.SMEM)] * n_smem
        + [pl.BlockSpec(memory_space=pltpu.VMEM)] * n_vmem
        + [pl.BlockSpec(memory_space=pltpu.HBM)] * n_hbm,
        out_specs=jax.tree.map(lambda _: pl.BlockSpec(memory_space=out_space), outs),
        scratch_shapes=scratch,
        compiler_params=pltpu.CompilerParams(vmem_limit_bytes=VMEM_LIMIT),
    )


def info_kernel(rows, weights, out):
    info = jnp.concatenate([rows[...].astype(F32), weights[...]], axis=1)
    for d in range(out.shape[0]):
        out[d] = info


def in_place(infos):
    count = infos.shape[0] // 4
    pieces = [infos[j * count : (j + 1) * count] for j in range(4)]
    pair, half = lax.axis_index("pair") == 0, lax.axis_index("half") == 0
    halves = [
        jnp.concatenate([jnp.where(pair, a, b), jnp.where(pair, b, a)], axis=0)
        for a, b in (pieces[:2], pieces[2:])
    ]
    a, b = halves
    return jnp.concatenate([jnp.where(half, a, b), jnp.where(half, b, a)], axis=0)


def contribution_kernel(
    slots, degrees, halves, orders_in, radial_in, spectrum_in, legendre_in, out,
    orders, radial, spectrum, legendre, turned, held, small, sems, outs
):
    parts = spectrum.shape[0]
    ways = sems.shape[1]
    step = spectrum.shape[1] // ways
    sides = [(legendre_in, legendre)] + [(spectrum_in.at[c], spectrum.at[c]) for c in range(parts)]
    copies = [
        [
            pltpu.make_async_copy(
                source.at[pl.ds(w * step, step)], target.at[pl.ds(w * step, step)], sems.at[c, w]
            )
            for w in range(ways)
        ]
        for c, (source, target) in enumerate(sides)
    ]
    first_copies = [
        pltpu.make_async_copy(orders_in, orders, small.at[0]),
        pltpu.make_async_copy(radial_in, radial, small.at[1]),
    ]
    for copy in first_copies:
        copy.start()
    for some in copies:
        for copy in some:
            copy.start()
    for copy in first_copies + copies[0]:
        copy.wait()
    turned[...] = jnp.transpose(legendre[...])
    levels_n = radial.shape[0]
    columns = levels_n * parts
    width = columns * slots
    rows = slots * degrees
    repeat = (iota((columns, levels_n), 0) // parts == iota((columns, levels_n), 1)).astype(BF16)
    repeated = dot(repeat, radial[...])
    part_of = iota(repeated.shape, 0) % parts
    levels = jnp.zeros((rows, columns), F32)
    for c in range(parts):
        table = jnp.where(part_of == c, repeated, 0.0).astype(BF16)
        for copy in copies[c + 1]:
            copy.wait()
        levels += dot_dims(spectrum[c], table, 1, 1)
    spread = (iota((columns, width), 0) == iota((columns, width), 1) // slots).astype(BF16)
    expanded = dot(levels.astype(BF16), spread)
    slot_of_lane = iota((degrees, width), 1) % slots
    degree = iota((degrees, width), 0) + lax.axis_index(("half", "z")) * degrees
    first_slot = lax.axis_index(MA) * slots
    blocks = []
    for k in range(slots):
        kept = (slot_of_lane == k) & (degree >= orders[first_slot + k])
        blocks.append(jnp.where(kept, expanded[k * degrees : (k + 1) * degrees], 0.0).astype(BF16))
    diagonal = jnp.concatenate(blocks, axis=0)
    n_z, lats, _ = out.shape
    block = lats // halves
    group = LANES // block
    writes = []
    for first in range(0, halves * n_z, group):
        lanes = slice(first * block, (first + group) * block)
        held[lanes] = dot(turned[lanes], diagonal).astype(BF16)
        for g in range(first, first + group):
            h, z = divmod(g, n_z)
            write = pltpu.make_async_copy(
                held.at[pl.ds(g * block, block)], out.at[z, pl.ds(h * block, block)], outs.at[g]
            )
            write.start()
            writes.append(write)
    for write in writes:
        write.wait()


def table_kernel(orders, cosines, sines):
    count = orders.shape[1]
    order = jnp.broadcast_to(as_column(orders[...], count), (count, LANES))
    angle = (order * iota((count, LANES), 1) & (NPHI - 1)).astype(F32) * (2.0 * math.pi / NPHI)
    weight = jnp.where(order == 0, 1.0, 2.0).astype(F32) / math.sqrt(NS)
    cosine, sine = jnp.cos(angle) * weight, jnp.sin(angle) * weight
    half_root = math.sqrt(0.5)
    for j in range(NPHI // LANES):
        eighth = order * j & 7
        size = jnp.where(eighth & 1 == 1, half_root, 1.0)
        turn_cos = jnp.where(eighth & 3 == 2, 0.0, jnp.where((eighth >= 3) & (eighth <= 5), -size, size))
        turn_sin = jnp.where(eighth & 3 == 0, 0.0, jnp.where(eighth > 4, -size, size))
        at = slice(j * LANES, (j + 1) * LANES)
        cosines[:, at] = (cosine * turn_cos - sine * turn_sin).astype(BF16)
        sines[:, at] = (-sine * turn_cos - cosine * turn_sin).astype(BF16)


def choice_kernel(per, infos, picks):
    lats = infos.shape[0]
    levels_n = infos.shape[1] // 2
    info = in_place(infos[...])
    q = iota((per, info.shape[1]), 0)
    own_level = (q == iota(q.shape, 1)) & (q < levels_n)
    wanted = [
        jnp.sum(jnp.where(own_level, info[t : t + 1], 0.0), axis=1, keepdims=True)
        for t in range(lats)
    ]
    absent = iota((lats * per, 1), 0) % per >= levels_n
    row = jnp.where(absent, -1.0, jnp.concatenate(wanted, axis=0))
    picks[...] = matches(row, iota(picks.shape, 1).astype(F32))


def column_kernel(per, arrived, infos, copies, base):
    lats = arrived.shape[1]
    levels_n = infos.shape[1] // 2
    width = arrived.shape[2] // levels_n
    total = arrived[0].astype(F32)
    for d in range(1, arrived.shape[0]):
        total += arrived[d].astype(F32)
    points = jnp.concatenate(
        [total[:, r * width : (r + 1) * width] for r in range(levels_n)], axis=0
    ).astype(BF16)
    info = in_place(infos[...])
    rows = jnp.concatenate([info[:, r : r + 1] for r in range(levels_n)], axis=0)
    weight = jnp.concatenate([info[:, r : r + 1] for r in range(levels_n, 2 * levels_n)], axis=0)
    onehot = matches(rows, iota((lats * levels_n, NS), 1).astype(F32))
    half = width // 2
    exact = points.astype(F32)
    weighted = (exact[:, :half] - COMPOSITION_WEIGHT * exact[:, half:]) * weight
    high = weighted.astype(BF16)
    low = (weighted - high.astype(F32)).astype(BF16)
    both = dot_dims(jnp.concatenate([high, low], axis=1), onehot, 0, 0)
    column = (both[:half] + both[half:]).astype(BF16)
    copies[...] = jnp.broadcast_to(column[None], copies.shape)
    stacked = jnp.concatenate([jnp.zeros_like(points), points], axis=1)
    point = iota((1, lats * levels_n), 1)
    places = matches(iota((lats * per, 1), 0), point % lats * per + point // lats)
    base[...] = dot(places, stacked).astype(BF16)


def select_kernel(levels_n, parts, step, picks, base, out):
    column = parts[0].astype(F32)
    for d in range(1, parts.shape[0]):
        column += parts[d].astype(F32)
    half = column.shape[0] // 2
    outward = as_column(step[...], step.shape[1]) * jnp.concatenate(
        [column[half:], column[:half]], axis=0
    )
    at = iota(column.shape, 1)
    after = jnp.where(at == NS - 1, 0.0, pltpu.roll(column, NS - 1, axis=1))
    before = jnp.where(at == 0, 0.0, pltpu.roll(column, 1, axis=1))
    around = after - before
    zeros = jnp.zeros_like(column)
    points = jnp.concatenate([outward, around, zeros, zeros], axis=0).astype(BF16)
    group = at // 4 % 4
    rows = jnp.concatenate([jnp.where(group == g, column, 0.0) for g in range(4)], axis=0)
    chosen = dot_dims(picks[...], points, 1, 1)
    per = out.shape[1]
    own = per - levels_n
    message = iota((picks.shape[0], 1), 0)
    level = message % per
    code = jnp.where(level >= levels_n, message // per % (NS // per) * own + level - levels_n, -1)
    s = iota((1, NS), 1)
    chosen += dot_dims(matches(code, s // per * own + s % own), rows.astype(BF16), 1, 1)
    chosen += base[...].astype(F32)
    out[...] = chosen.astype(BF16).reshape(out.shape)


def advect_kernel(levels_n, slots, got, cosines, sines, slope, radius, owned, advected):
    n_ma, per, _ = got.shape[1:]
    taken = [(got[0, b].astype(F32) + got[1, b].astype(F32)).astype(BF16) for b in range(n_ma)]
    by_part = []
    for i in range(2):
        groups = []
        for g in range(4):
            at = (2 * g + i) * slots
            groups.append(jnp.concatenate([x[:, at : at + slots] for x in taken], axis=1))
        by_part.append(groups)
    scale = slope[...]
    sides = []
    for i in range(2):
        turned = [
            (by_part[1 - i][g].astype(F32) * (scale if i else -scale)).astype(BF16) for g in (2, 3)
        ]
        sides.append(jnp.concatenate(by_part[i] + turned, axis=0))
    result = dot(sides[0], cosines[...]) + dot(sides[1], sines[...])
    rows = [result[g * per : g * per + levels_n] for g in range(6)]
    inverse = 1.0 / as_column(radius[...], levels_n)
    outward = rows[0] * (0.5 * inverse)
    around = -0.5 * rows[1]
    held = [x.astype(BF16).astype(F32) for x in rows[2:]]
    for f in range(2):
        field, side = held[f], held[2 + f]
        value = field - (TIME_STEP * inverse) * (around * side + outward * field)
        for r in range(levels_n):
            advected[f, r] = value[r : r + 1]
    mine = jnp.concatenate([result[g * per + levels_n : (g + 1) * per] for g in range(4)], axis=0)
    width = owned.shape[1]
    start = lax.axis_index(("half", "z")) * width
    mine = pltpu.roll(mine, lax.rem(NPHI - start, NPHI), axis=1)
    owned[...] = mine[:, :width]


def in_hbm(array):
    return pltpu.with_memory_space_constraint(array, pltpu.HBM)


def exchanged(blocks, axis):
    return lax.all_to_all(blocks, axis, split_axis=0, concat_axis=0, tiled=True)


def on_device(spectrum, radial_table, legendre, order_table, cylinder_row, column_weight):
    parts, slots, degrees, modes = spectrum.shape
    levels_n = radial_table.shape[0]
    lats = legendre.shape[2]
    n_z = lax.axis_size("z")
    n_half = lax.axis_size("half")
    n_ma = lax.axis_size(MA)
    lat_block = lats // n_z
    row_block = NS // n_ma
    lon_block = NPHI // (n_half * n_z)
    me_ma = lax.axis_index(MA)
    swap = [(0, 1), (1, 0)]

    near = ("y", "x")
    info = vmem_call(
        info_kernel,
        pltpu.HBM((lax.axis_size(near), 1, 2 * levels_n), F32),
        0, 2,
    )(in_hbm(cylinder_row), in_hbm(column_weight))
    info = exchanged(info, near).reshape(-1, 2 * levels_n)
    contribution = vmem_call(
        functools.partial(contribution_kernel, slots, degrees, n_half),
        pltpu.HBM((n_z, lat_block, levels_n * parts * slots), BF16),
        0, 0, 4,
        (
            pltpu.SMEM(order_table.shape, I32),
            pltpu.VMEM(radial_table.shape, BF16),
            pltpu.VMEM((parts, slots * degrees, modes), BF16),
            pltpu.VMEM((slots * degrees, lats), BF16),
            pltpu.VMEM((lats, slots * degrees), BF16),
            pltpu.VMEM((lats, levels_n * parts * slots), BF16),
            pltpu.SemaphoreType.DMA((2,)),
            pltpu.SemaphoreType.DMA((parts + 1, 4)),
            pltpu.SemaphoreType.DMA((n_half * n_z,)),
        ),
        pltpu.HBM,
    )(
        in_hbm(order_table),
        in_hbm(radial_table),
        in_hbm(spectrum.reshape(parts, slots * degrees, modes)),
        in_hbm(legendre.reshape(slots * degrees, lats)),
    )
    arrived = exchanged(contribution, "z")
    info = lax.all_gather(info, "core", axis=1).reshape(-1, 2 * levels_n)
    info = jnp.concatenate([info, lax.ppermute(info, "pair", swap)], axis=0)
    infos = jnp.concatenate([info, lax.ppermute(info, "half", swap)], axis=0)
    my_orders = lax.dynamic_slice_in_dim(order_table, me_ma * slots, slots)
    step = 2.0 * jnp.sin(my_orders.astype(F32) * (2.0 * math.pi / NPHI))
    step = jnp.concatenate([-step, step]).reshape(1, -1)
    slope = (order_table.astype(F32) / NS).reshape(1, -1)
    radius = (0.35 + 0.65 * (cylinder_row.astype(F32) + 0.5) / NS).reshape(1, -1)
    table = jax.ShapeDtypeStruct((lats, NPHI), BF16)
    cosines, sines = vmem_call(table_kernel, (table, table), 0, 1)(order_table.reshape(1, -1))
    messages = lat_block * row_block
    picks = vmem_call(
        functools.partial(choice_kernel, row_block),
        jax.ShapeDtypeStruct((messages, NS), BF16),
        0, 1,
    )(infos)
    arrived, cosines, sines, step, slope, radius, infos, picks = lax.optimization_barrier(
        (arrived, cosines, sines, step, slope, radius, infos, picks)
    )
    copies, base = vmem_call(
        functools.partial(column_kernel, row_block),
        (
            jax.ShapeDtypeStruct((n_z, 2 * slots, NS), BF16),
            jax.ShapeDtypeStruct((messages, LANES), BF16),
        ),
        0, 2,
    )(arrived, infos)
    partials = exchanged(copies, "z")
    chosen = vmem_call(
        functools.partial(select_kernel, levels_n),
        jax.ShapeDtypeStruct((lat_block, row_block, LANES), BF16),
        0, 4,
    )(partials, step, picks, base)
    got = exchanged(chosen, ("half", *MA)).reshape(n_half, n_ma, row_block, LANES)
    owned, advected = vmem_call(
        functools.partial(advect_kernel, levels_n, slots),
        (
            jax.ShapeDtypeStruct((row_block, lon_block), F32),
            jax.ShapeDtypeStruct((2, levels_n, 1, NPHI), F32),
        ),
        0, 5,
    )(got, cosines, sines, slope, radius)
    return (owned, jnp.swapaxes(advected, 1, 2))


def solution(mesh):
    parts = Mesh(
        mesh.devices.reshape(HALVES, -1, PAIRS, PAIRS, mesh.shape["ma"] // 8, 2),
        ("half", "z", *MA),
    )
    rad = ("half", "z")
    return jax.shard_map(
        on_device,
        mesh=parts,
        in_specs=(
            P(None, MA, rad, None),
            P(),
            P(MA, rad, None),
            P(),
            P((*rad, *MA), None),
            P((*rad, *MA), None),
        ),
        out_specs=(P(MA, rad), P(None, (*rad, *MA), None, None)),
        check_vma=False,
    )
```

```python
import functools
import math

import jax
import jax.numpy as jnp
from jax import lax
from jax.experimental import pallas as pl
from jax.experimental.pallas import tpu as pltpu
from jax.sharding import Mesh
from jax.sharding import PartitionSpec as P

NPHI = 1024
NS = 512
LANES = 128
HALVES = 2
PAIRS = 2
MA = ("pair", "y", "x", "core")
VMEM_LIMIT = 20 * 2**20
TIME_STEP = 0.05
COMPOSITION_WEIGHT = 0.8
BF16 = jnp.bfloat16
F32 = jnp.float32
I32 = jnp.int32

dot = functools.partial(jnp.dot, preferred_element_type=F32)


def iota(shape, dim):
    return lax.broadcasted_iota(I32, shape, dim)


def as_column(row, width):
    return jnp.transpose(jnp.broadcast_to(row, (8, width)))[:, :1]


def matches(column, row):
    return (column == row).astype(F32).astype(BF16)


def dot_dims(x, y, dim_x, dim_y):
    return lax.dot_general(x, y, (((dim_x,), (dim_y,)), ((), ())), preferred_element_type=F32)


def vmem_call(body, outs, n_smem, n_vmem, n_hbm=0, scratch=(), out_space=pltpu.VMEM, cost=None):
    return pl.pallas_call(
        body,
        out_shape=outs,
        in_specs=[pl.BlockSpec(memory_space=pltpu.SMEM)] * n_smem
        + [pl.BlockSpec(memory_space=pltpu.VMEM)] * n_vmem
        + [pl.BlockSpec(memory_space=pltpu.HBM)] * n_hbm,
        out_specs=jax.tree.map(lambda _: pl.BlockSpec(memory_space=out_space), outs),
        scratch_shapes=scratch,
        cost_estimate=cost,
        compiler_params=pltpu.CompilerParams(vmem_limit_bytes=VMEM_LIMIT),
    )


def info_kernel(rows, weights, out):
    info = jnp.concatenate([rows[...].astype(F32), weights[...]], axis=1)
    for d in range(out.shape[0]):
        out[d] = info


def in_place(infos):
    count = infos.shape[0] // 4
    pieces = [infos[j * count : (j + 1) * count] for j in range(4)]
    pair, half = lax.axis_index("pair") == 0, lax.axis_index("half") == 0
    halves = [
        jnp.concatenate([jnp.where(pair, a, b), jnp.where(pair, b, a)], axis=0)
        for a, b in (pieces[:2], pieces[2:])
    ]
    a, b = halves
    return jnp.concatenate([jnp.where(half, a, b), jnp.where(half, b, a)], axis=0)


def contribution_kernel(
    slots, degrees, halves, spectrum, legendre, orders_in, radial_in, out,
    orders, radial, held, small, outs
):
    parts = spectrum.shape[0]
    copies = [
        pltpu.make_async_copy(orders_in, orders, small.at[0]),
        pltpu.make_async_copy(radial_in, radial, small.at[1]),
    ]
    for copy in copies:
        copy.start()
    for copy in copies:
        copy.wait()
    levels_n = radial.shape[0]
    columns = levels_n * parts
    width = columns * slots
    rows = slots * degrees
    repeat = (iota((columns, levels_n), 0) // parts == iota((columns, levels_n), 1)).astype(BF16)
    repeated = dot(repeat, radial[...])
    part_of = iota(repeated.shape, 0) % parts
    levels = jnp.zeros((rows, columns), F32)
    for c in range(parts):
        table = jnp.where(part_of == c, repeated, 0.0).astype(BF16)
        levels += dot_dims(spectrum[c], table, 1, 1)
    spread = (iota((columns, width), 0) == iota((columns, width), 1) // slots).astype(BF16)
    expanded = dot(levels.astype(BF16), spread)
    slot_of_lane = iota((degrees, width), 1) % slots
    degree = iota((degrees, width), 0) + lax.axis_index(("half", "z")) * degrees
    first_slot = lax.axis_index(MA) * slots
    blocks = []
    for k in range(slots):
        kept = (slot_of_lane == k) & (degree >= orders[first_slot + k])
        blocks.append(jnp.where(kept, expanded[k * degrees : (k + 1) * degrees], 0.0).astype(BF16))
    diagonal = jnp.concatenate(blocks, axis=0)
    n_z, lats, _ = out.shape
    block = lats // halves
    group = LANES // block
    writes = []
    for first in range(0, halves * n_z, group):
        lanes = slice(first * block, (first + group) * block)
        held[lanes] = dot_dims(legendre[:, lanes], diagonal, 0, 0).astype(BF16)
        for g in range(first, first + group):
            h, z = divmod(g, n_z)
            write = pltpu.make_async_copy(
                held.at[pl.ds(g * block, block)], out.at[z, pl.ds(h * block, block)], outs.at[g]
            )
            write.start()
            writes.append(write)
    for write in writes:
        write.wait()


def table_kernel(orders, cosines, sines):
    count = orders.shape[1]
    order = jnp.broadcast_to(as_column(orders[...], count), (count, LANES))
    angle = (order * iota((count, LANES), 1) & (NPHI - 1)).astype(F32) * (2.0 * math.pi / NPHI)
    weight = jnp.where(order == 0, 1.0, 2.0).astype(F32) / math.sqrt(NS)
    cosine, sine = jnp.cos(angle) * weight, jnp.sin(angle) * weight
    half_root = math.sqrt(0.5)
    for j in range(NPHI // LANES):
        eighth = order * j & 7
        size = jnp.where(eighth & 1 == 1, half_root, 1.0)
        turn_cos = jnp.where(eighth & 3 == 2, 0.0, jnp.where((eighth >= 3) & (eighth <= 5), -size, size))
        turn_sin = jnp.where(eighth & 3 == 0, 0.0, jnp.where(eighth > 4, -size, size))
        at = slice(j * LANES, (j + 1) * LANES)
        cosines[:, at] = (cosine * turn_cos - sine * turn_sin).astype(BF16)
        sines[:, at] = (-sine * turn_cos - cosine * turn_sin).astype(BF16)


def choice_kernel(per, infos, picks):
    lats = infos.shape[0]
    levels_n = infos.shape[1] // 2
    info = in_place(infos[...])
    q = iota((per, info.shape[1]), 0)
    own_level = (q == iota(q.shape, 1)) & (q < levels_n)
    wanted = [
        jnp.sum(jnp.where(own_level, info[t : t + 1], 0.0), axis=1, keepdims=True)
        for t in range(lats)
    ]
    absent = iota((lats * per, 1), 0) % per >= levels_n
    row = jnp.where(absent, -1.0, jnp.concatenate(wanted, axis=0))
    picks[...] = matches(row, iota(picks.shape, 1).astype(F32))


def column_kernel(per, arrived, infos, copies, base):
    lats = arrived.shape[1]
    levels_n = infos.shape[1] // 2
    width = arrived.shape[2] // levels_n
    total = arrived[0].astype(F32)
    for d in range(1, arrived.shape[0]):
        total += arrived[d].astype(F32)
    exact = jnp.concatenate(
        [total[:, r * width : (r + 1) * width] for r in range(levels_n)], axis=0
    )
    points = exact.astype(BF16)
    info = in_place(infos[...])
    rows = jnp.concatenate([info[:, r : r + 1] for r in range(levels_n)], axis=0)
    weight = jnp.concatenate([info[:, r : r + 1] for r in range(levels_n, 2 * levels_n)], axis=0)
    onehot = matches(rows, iota((lats * levels_n, NS), 1).astype(F32))
    half = width // 2
    weighted = (exact[:, :half] - COMPOSITION_WEIGHT * exact[:, half:]) * weight
    high = weighted.astype(BF16)
    low = (weighted - high.astype(F32)).astype(BF16)
    both = dot_dims(jnp.concatenate([high, low], axis=1), onehot, 0, 0)
    column = (both[:half] + both[half:]).astype(BF16)
    copies[...] = jnp.broadcast_to(column[None], copies.shape)
    stacked = jnp.concatenate([jnp.zeros_like(points), points], axis=1)
    point = iota((1, lats * levels_n), 1)
    places = matches(iota((lats * per, 1), 0), point % lats * per + point // lats)
    base[...] = dot(places, stacked).astype(BF16)


def select_kernel(levels_n, parts, step, picks, base, out):
    column = parts[0].astype(F32)
    for d in range(1, parts.shape[0]):
        column += parts[d].astype(F32)
    half = column.shape[0] // 2
    outward = as_column(step[...], step.shape[1]) * jnp.concatenate(
        [column[half:], column[:half]], axis=0
    )
    at = iota(column.shape, 1)
    after = jnp.where(at == NS - 1, 0.0, pltpu.roll(column, NS - 1, axis=1))
    before = jnp.where(at == 0, 0.0, pltpu.roll(column, 1, axis=1))
    around = after - before
    zeros = jnp.zeros_like(column)
    points = jnp.concatenate([outward, around, zeros, zeros], axis=0).astype(BF16)
    group = at // 4 % 4
    rows = jnp.concatenate([jnp.where(group == g, column, 0.0) for g in range(4)], axis=0)
    chosen = dot_dims(picks[...], points, 1, 1)
    per = out.shape[1]
    own = per - levels_n
    message = iota((picks.shape[0], 1), 0)
    level = message % per
    code = jnp.where(level >= levels_n, message // per % (NS // per) * own + level - levels_n, -1)
    s = iota((1, NS), 1)
    chosen += dot_dims(matches(code, s // per * own + s % own), rows.astype(BF16), 1, 1)
    chosen += base[...].astype(F32)
    out[...] = chosen.astype(BF16).reshape(out.shape)


def advect_kernel(levels_n, slots, got, cosines, sines, slope, radius, owned, advected):
    n_ma, per, _ = got.shape[1:]
    taken = [(got[0, b].astype(F32) + got[1, b].astype(F32)).astype(BF16) for b in range(n_ma)]
    by_part = []
    for i in range(2):
        groups = []
        for g in range(4):
            at = (2 * g + i) * slots
            groups.append(jnp.concatenate([x[:, at : at + slots] for x in taken], axis=1))
        by_part.append(groups)
    scale = slope[...]
    sides = []
    for i in range(2):
        turned = [
            (by_part[1 - i][g].astype(F32) * (scale if i else -scale)).astype(BF16) for g in (2, 3)
        ]
        sides.append(jnp.concatenate(by_part[i] + turned, axis=0))
    result = dot(sides[0], cosines[...]) + dot(sides[1], sines[...])
    rows = [result[g * per : g * per + levels_n] for g in range(6)]
    inverse = 1.0 / as_column(radius[...], levels_n)
    outward = rows[0] * (0.5 * inverse)
    around = -0.5 * rows[1]
    held = [x.astype(BF16).astype(F32) for x in rows[2:]]
    for f in range(2):
        field, side = held[f], held[2 + f]
        value = field - (TIME_STEP * inverse) * (around * side + outward * field)
        for r in range(levels_n):
            advected[f, r] = value[r : r + 1]
    mine = jnp.concatenate([result[g * per + levels_n : (g + 1) * per] for g in range(4)], axis=0)
    width = owned.shape[1]
    start = lax.axis_index(("half", "z")) * width
    mine = pltpu.roll(mine, lax.rem(NPHI - start, NPHI), axis=1)
    owned[...] = mine[:, :width]


def in_hbm(array):
    return pltpu.with_memory_space_constraint(array, pltpu.HBM)


def exchanged(blocks, axis):
    return lax.all_to_all(blocks, axis, split_axis=0, concat_axis=0, tiled=True)


def on_device(spectrum, radial_table, legendre, order_table, cylinder_row, column_weight):
    parts, slots, degrees, modes = spectrum.shape
    levels_n = radial_table.shape[0]
    lats = legendre.shape[2]
    n_z = lax.axis_size("z")
    n_half = lax.axis_size("half")
    n_ma = lax.axis_size(MA)
    lat_block = lats // n_z
    row_block = NS // n_ma
    lon_block = NPHI // (n_half * n_z)
    me_ma = lax.axis_index(MA)
    swap = [(0, 1), (1, 0)]

    near = ("y", "x")
    info = vmem_call(
        info_kernel,
        pltpu.HBM((lax.axis_size(near), 1, 2 * levels_n), F32),
        0, 2,
        cost=pl.CostEstimate(flops=4 * 10**9, bytes_accessed=4 * 10**7, transcendentals=0),
    )(in_hbm(cylinder_row), in_hbm(column_weight))
    info = exchanged(info, near).reshape(-1, 2 * levels_n)
    contribution = vmem_call(
        functools.partial(contribution_kernel, slots, degrees, n_half),
        pltpu.HBM((n_z, lat_block, levels_n * parts * slots), BF16),
        0, 2, 2,
        (
            pltpu.SMEM(order_table.shape, I32),
            pltpu.VMEM(radial_table.shape, BF16),
            pltpu.VMEM((lats, levels_n * parts * slots), BF16),
            pltpu.SemaphoreType.DMA((2,)),
            pltpu.SemaphoreType.DMA((n_half * n_z,)),
        ),
        pltpu.HBM,
    )(
        spectrum.reshape(parts, slots * degrees, modes),
        legendre.reshape(slots * degrees, lats),
        in_hbm(order_table),
        in_hbm(radial_table),
    )
    arrived = exchanged(contribution, "z")
    info = lax.all_gather(info, "core", axis=1).reshape(-1, 2 * levels_n)
    info = jnp.concatenate([info, lax.ppermute(info, "pair", swap)], axis=0)
    infos = jnp.concatenate([info, lax.ppermute(info, "half", swap)], axis=0)
    my_orders = lax.dynamic_slice_in_dim(order_table, me_ma * slots, slots)
    step = 2.0 * jnp.sin(my_orders.astype(F32) * (2.0 * math.pi / NPHI))
    step = jnp.concatenate([-step, step]).reshape(1, -1)
    slope = (order_table.astype(F32) / NS).reshape(1, -1)
    radius = (0.35 + 0.65 * (cylinder_row.astype(F32) + 0.5) / NS).reshape(1, -1)
    table = jax.ShapeDtypeStruct((lats, NPHI), BF16)
    cosines, sines = vmem_call(table_kernel, (table, table), 0, 1)(order_table.reshape(1, -1))
    messages = lat_block * row_block
    picks = vmem_call(
        functools.partial(choice_kernel, row_block),
        jax.ShapeDtypeStruct((messages, NS), BF16),
        0, 1,
    )(infos)
    arrived, cosines, sines, step, slope, radius, infos, picks = lax.optimization_barrier(
        (arrived, cosines, sines, step, slope, radius, infos, picks)
    )
    copies, base = vmem_call(
        functools.partial(column_kernel, row_block),
        (
            jax.ShapeDtypeStruct((n_z, 2 * slots, NS), BF16),
            jax.ShapeDtypeStruct((messages, LANES), BF16),
        ),
        0, 2,
    )(arrived, infos)
    partials = exchanged(copies, "z")
    chosen = vmem_call(
        functools.partial(select_kernel, levels_n),
        jax.ShapeDtypeStruct((lat_block, row_block, LANES), BF16),
        0, 4,
    )(partials, step, picks, base)
    got = exchanged(chosen, ("half", *MA)).reshape(n_half, n_ma, row_block, LANES)
    owned, advected = vmem_call(
        functools.partial(advect_kernel, levels_n, slots),
        (
            jax.ShapeDtypeStruct((row_block, lon_block), F32),
            jax.ShapeDtypeStruct((2, levels_n, 1, NPHI), F32),
        ),
        0, 5,
    )(got, cosines, sines, slope, radius)
    return (owned, jnp.swapaxes(advected, 1, 2))


def solution(mesh):
    parts = Mesh(
        mesh.devices.reshape(HALVES, -1, PAIRS, PAIRS, mesh.shape["ma"] // 8, 2),
        ("half", "z", *MA),
    )
    rad = ("half", "z")
    return jax.shard_map(
        on_device,
        mesh=parts,
        in_specs=(
            P(None, MA, rad, None),
            P(),
            P(MA, rad, None),
            P(),
            P((*rad, *MA), None),
            P((*rad, *MA), None),
        ),
        out_specs=(P(MA, rad), P(None, (*rad, *MA), None, None)),
        check_vma=False,
    )
```

```python
import functools
import math

import jax
import jax.numpy as jnp
from jax import lax
from jax.experimental import pallas as pl
from jax.experimental.pallas import tpu as pltpu
from jax.sharding import Mesh
from jax.sharding import PartitionSpec as P

NPHI = 1024
NS = 512
LANES = 128
HALVES = 2
PAIRS = 2
MA = ("pair", "y", "x", "core")
VMEM_LIMIT = 20 * 2**20
TIME_STEP = 0.05
COMPOSITION_WEIGHT = 0.8
BF16 = jnp.bfloat16
F32 = jnp.float32
I32 = jnp.int32

dot = functools.partial(jnp.dot, preferred_element_type=F32)


def iota(shape, dim):
    return lax.broadcasted_iota(I32, shape, dim)


def as_column(row, width):
    return jnp.transpose(jnp.broadcast_to(row, (8, width)))[:, :1]


def matches(column, row):
    return (column == row).astype(F32).astype(BF16)


def dot_dims(x, y, dim_x, dim_y):
    return lax.dot_general(x, y, (((dim_x,), (dim_y,)), ((), ())), preferred_element_type=F32)


def vmem_call(body, outs, n_smem, n_vmem, n_hbm=0, scratch=(), out_space=pltpu.VMEM, cost=None):
    return pl.pallas_call(
        body,
        out_shape=outs,
        in_specs=[pl.BlockSpec(memory_space=pltpu.SMEM)] * n_smem
        + [pl.BlockSpec(memory_space=pltpu.VMEM)] * n_vmem
        + [pl.BlockSpec(memory_space=pltpu.HBM)] * n_hbm,
        out_specs=jax.tree.map(lambda _: pl.BlockSpec(memory_space=out_space), outs),
        scratch_shapes=scratch,
        cost_estimate=cost,
        compiler_params=pltpu.CompilerParams(vmem_limit_bytes=VMEM_LIMIT),
    )


def info_kernel(rows, weights, out):
    info = jnp.concatenate([rows[...].astype(F32), weights[...]], axis=1)
    for d in range(out.shape[0]):
        out[d] = info


def in_place(infos):
    count = infos.shape[0] // 4
    pieces = [infos[j * count : (j + 1) * count] for j in range(4)]
    pair, half = lax.axis_index("pair") == 0, lax.axis_index("half") == 0
    halves = [
        jnp.concatenate([jnp.where(pair, a, b), jnp.where(pair, b, a)], axis=0)
        for a, b in (pieces[:2], pieces[2:])
    ]
    a, b = halves
    return jnp.concatenate([jnp.where(half, a, b), jnp.where(half, b, a)], axis=0)


def contribution_kernel(
    slots, degrees, halves, spectrum, legendre, orders_in, radial_in, out,
    orders, radial, held, small, outs
):
    parts = spectrum.shape[0]
    copies = [
        pltpu.make_async_copy(orders_in, orders, small.at[0]),
        pltpu.make_async_copy(radial_in, radial, small.at[1]),
    ]
    for copy in copies:
        copy.start()
    for copy in copies:
        copy.wait()
    levels_n = radial.shape[0]
    columns = levels_n * parts
    width = columns * slots
    rows = slots * degrees
    repeat = (iota((columns, levels_n), 0) // parts == iota((columns, levels_n), 1)).astype(BF16)
    repeated = dot(repeat, radial[...])
    part_of = iota(repeated.shape, 0) % parts
    levels = jnp.zeros((rows, columns), F32)
    for c in range(parts):
        table = jnp.where(part_of == c, repeated, 0.0).astype(BF16)
        levels += dot_dims(spectrum[c], table, 1, 1)
    spread = (iota((columns, width), 0) == iota((columns, width), 1) // slots).astype(BF16)
    expanded = dot(levels.astype(BF16), spread)
    slot_of_lane = iota((degrees, width), 1) % slots
    degree = iota((degrees, width), 0) + lax.axis_index(("half", "z")) * degrees
    first_slot = lax.axis_index(MA) * slots
    blocks = []
    for k in range(slots):
        kept = (slot_of_lane == k) & (degree >= orders[first_slot + k])
        blocks.append(jnp.where(kept, expanded[k * degrees : (k + 1) * degrees], 0.0).astype(BF16))
    diagonal = jnp.concatenate(blocks, axis=0)
    n_z, lats, _ = out.shape
    block = lats // halves
    group = LANES // block
    writes = []
    for first in range(0, halves * n_z, group):
        lanes = slice(first * block, (first + group) * block)
        held[lanes] = dot_dims(legendre[:, lanes], diagonal, 0, 0).astype(BF16)
        for g in range(first, first + group):
            h, z = divmod(g, n_z)
            write = pltpu.make_async_copy(
                held.at[pl.ds(g * block, block)], out.at[z, pl.ds(h * block, block)], outs.at[g]
            )
            write.start()
            writes.append(write)
    for write in writes:
        write.wait()


def table_kernel(orders, cosines, sines):
    count = orders.shape[1]
    column = as_column(orders[...], count)
    half_root = math.sqrt(0.5)
    some = 64
    for first in range(0, count, some):
        rows = slice(first, first + some)
        order = jnp.broadcast_to(column[rows], (some, LANES))
        phase = order * iota((some, LANES), 1) & (NPHI - 1)
        angle = phase.astype(F32) * (2.0 * math.pi / NPHI)
        weight = jnp.where(order == 0, 1.0, 2.0).astype(F32) / math.sqrt(NS)
        cosine, sine = jnp.cos(angle) * weight, jnp.sin(angle) * weight
        eighth = order & 7
        size = jnp.where(eighth & 1 == 1, half_root, 1.0)
        turn_cos = jnp.where(eighth & 3 == 2, 0.0, jnp.where((eighth >= 3) & (eighth <= 5), -size, size))
        turn_sin = jnp.where(eighth & 3 == 0, 0.0, jnp.where(eighth > 4, -size, size))
        for j in range(NPHI // LANES):
            at = slice(j * LANES, (j + 1) * LANES)
            cosines[rows, at] = cosine.astype(BF16)
            sines[rows, at] = (-sine).astype(BF16)
            cosine, sine = cosine * turn_cos - sine * turn_sin, sine * turn_cos + cosine * turn_sin


def choice_kernel(per, infos, picks):
    lats = infos.shape[0]
    levels_n = infos.shape[1] // 2
    info = in_place(infos[...])
    q = iota((per, info.shape[1]), 0)
    own_level = (q == iota(q.shape, 1)) & (q < levels_n)
    wanted = [
        jnp.sum(jnp.where(own_level, info[t : t + 1], 0.0), axis=1, keepdims=True)
        for t in range(lats)
    ]
    absent = iota((lats * per, 1), 0) % per >= levels_n
    row = jnp.where(absent, -1.0, jnp.concatenate(wanted, axis=0))
    picks[...] = matches(row, iota(picks.shape, 1).astype(F32))


def column_kernel(per, arrived, infos, copies, base):
    lats = arrived.shape[1]
    levels_n = infos.shape[1] // 2
    width = arrived.shape[2] // levels_n
    total = arrived[0].astype(F32)
    for d in range(1, arrived.shape[0]):
        total += arrived[d].astype(F32)
    exact = jnp.concatenate(
        [total[:, r * width : (r + 1) * width] for r in range(levels_n)], axis=0
    )
    points = exact.astype(BF16)
    info = in_place(infos[...])
    rows = jnp.concatenate([info[:, r : r + 1] for r in range(levels_n)], axis=0)
    weight = jnp.concatenate([info[:, r : r + 1] for r in range(levels_n, 2 * levels_n)], axis=0)
    onehot = matches(rows, iota((lats * levels_n, NS), 1).astype(F32))
    half = width // 2
    weighted = (exact[:, :half] - COMPOSITION_WEIGHT * exact[:, half:]) * weight
    high = weighted.astype(BF16)
    low = (weighted - high.astype(F32)).astype(BF16)
    both = dot_dims(jnp.concatenate([high, low], axis=1), onehot, 0, 0)
    column = (both[:half] + both[half:]).astype(BF16)
    copies[...] = jnp.broadcast_to(column[None], copies.shape)
    stacked = jnp.concatenate([jnp.zeros_like(points), points], axis=1)
    point = iota((1, lats * levels_n), 1)
    places = matches(iota((lats * per, 1), 0), point % lats * per + point // lats)
    base[...] = dot(places, stacked).astype(BF16)


def select_kernel(levels_n, parts, step, picks, base, out):
    column = parts[0].astype(F32)
    for d in range(1, parts.shape[0]):
        column += parts[d].astype(F32)
    half = column.shape[0] // 2
    outward = as_column(step[...], step.shape[1]) * jnp.concatenate(
        [column[half:], column[:half]], axis=0
    )
    at = iota(column.shape, 1)
    after = jnp.where(at == NS - 1, 0.0, pltpu.roll(column, NS - 1, axis=1))
    before = jnp.where(at == 0, 0.0, pltpu.roll(column, 1, axis=1))
    around = after - before
    zeros = jnp.zeros_like(column)
    points = jnp.concatenate([outward, around, zeros, zeros], axis=0).astype(BF16)
    group = at // 4 % 4
    rows = jnp.concatenate([jnp.where(group == g, column, 0.0) for g in range(4)], axis=0)
    chosen = dot_dims(picks[...], points, 1, 1)
    per = out.shape[1]
    own = per - levels_n
    message = iota((picks.shape[0], 1), 0)
    level = message % per
    code = jnp.where(level >= levels_n, message // per % (NS // per) * own + level - levels_n, -1)
    s = iota((1, NS), 1)
    chosen += dot_dims(matches(code, s // per * own + s % own), rows.astype(BF16), 1, 1)
    chosen += base[...].astype(F32)
    out[...] = chosen.astype(BF16).reshape(out.shape)


def advect_kernel(levels_n, slots, got, cosines, sines, slope, radius, owned, advected):
    n_ma, per, _ = got.shape[1:]
    taken = [(got[0, b].astype(F32) + got[1, b].astype(F32)).astype(BF16) for b in range(n_ma)]
    by_part = []
    for i in range(2):
        groups = []
        for g in range(4):
            at = (2 * g + i) * slots
            groups.append(jnp.concatenate([x[:, at : at + slots] for x in taken], axis=1))
        by_part.append(groups)
    scale = slope[...]
    sides = []
    for i in range(2):
        turned = [
            (by_part[1 - i][g].astype(F32) * (scale if i else -scale)).astype(BF16) for g in (2, 3)
        ]
        sides.append(jnp.concatenate(by_part[i] + turned, axis=0))
    result = dot(sides[0], cosines[...]) + dot(sides[1], sines[...])
    rows = [result[g * per : g * per + levels_n] for g in range(6)]
    inverse = 1.0 / as_column(radius[...], levels_n)
    outward = rows[0] * (0.5 * inverse)
    around = -0.5 * rows[1]
    held = [x.astype(BF16).astype(F32) for x in rows[2:]]
    for f in range(2):
        field, side = held[f], held[2 + f]
        value = field - (TIME_STEP * inverse) * (around * side + outward * field)
        for r in range(levels_n):
            advected[f, r] = value[r : r + 1]
    mine = jnp.concatenate([result[g * per + levels_n : (g + 1) * per] for g in range(4)], axis=0)
    width = owned.shape[1]
    start = lax.axis_index(("half", "z")) * width
    mine = pltpu.roll(mine, lax.rem(NPHI - start, NPHI), axis=1)
    owned[...] = mine[:, :width]


def in_hbm(array):
    return pltpu.with_memory_space_constraint(array, pltpu.HBM)


def exchanged(blocks, axis):
    return lax.all_to_all(blocks, axis, split_axis=0, concat_axis=0, tiled=True)


def on_device(spectrum, radial_table, legendre, order_table, cylinder_row, column_weight):
    parts, slots, degrees, modes = spectrum.shape
    levels_n = radial_table.shape[0]
    lats = legendre.shape[2]
    n_z = lax.axis_size("z")
    n_half = lax.axis_size("half")
    n_ma = lax.axis_size(MA)
    lat_block = lats // n_z
    row_block = NS // n_ma
    lon_block = NPHI // (n_half * n_z)
    me_ma = lax.axis_index(MA)
    swap = [(0, 1), (1, 0)]

    near = ("x", "core")
    info = vmem_call(
        info_kernel,
        pltpu.HBM((lax.axis_size(near), 1, 2 * levels_n), F32),
        0, 2,
        cost=pl.CostEstimate(flops=4 * 10**9, bytes_accessed=4 * 10**7, transcendentals=0),
    )(in_hbm(cylinder_row), in_hbm(column_weight))
    info = exchanged(info, near).reshape(-1, 2 * levels_n)
    contribution = vmem_call(
        functools.partial(contribution_kernel, slots, degrees, n_half),
        pltpu.HBM((n_z, lat_block, levels_n * parts * slots), BF16),
        0, 2, 2,
        (
            pltpu.SMEM(order_table.shape, I32),
            pltpu.VMEM(radial_table.shape, BF16),
            pltpu.VMEM((lats, levels_n * parts * slots), BF16),
            pltpu.SemaphoreType.DMA((2,)),
            pltpu.SemaphoreType.DMA((n_half * n_z,)),
        ),
        pltpu.HBM,
    )(
        spectrum.reshape(parts, slots * degrees, modes),
        legendre.reshape(slots * degrees, lats),
        in_hbm(order_table),
        in_hbm(radial_table),
    )
    arrived = exchanged(contribution, "z")
    info = lax.all_gather(info, "y", axis=0, tiled=True)
    info = jnp.concatenate([info, lax.ppermute(info, "pair", swap)], axis=0)
    infos = jnp.concatenate([info, lax.ppermute(info, "half", swap)], axis=0)
    my_orders = lax.dynamic_slice_in_dim(order_table, me_ma * slots, slots)
    step = 2.0 * jnp.sin(my_orders.astype(F32) * (2.0 * math.pi / NPHI))
    step = jnp.concatenate([-step, step]).reshape(1, -1)
    slope = (order_table.astype(F32) / NS).reshape(1, -1)
    radius = (0.35 + 0.65 * (cylinder_row.astype(F32) + 0.5) / NS).reshape(1, -1)
    table = jax.ShapeDtypeStruct((lats, NPHI), BF16)
    cosines, sines = vmem_call(table_kernel, (table, table), 0, 1)(order_table.reshape(1, -1))
    messages = lat_block * row_block
    picks = vmem_call(
        functools.partial(choice_kernel, row_block),
        jax.ShapeDtypeStruct((messages, NS), BF16),
        0, 1,
    )(infos)
    arrived, cosines, sines, step, slope, radius, infos, picks = lax.optimization_barrier(
        (arrived, cosines, sines, step, slope, radius, infos, picks)
    )
    copies, base = vmem_call(
        functools.partial(column_kernel, row_block),
        (
            jax.ShapeDtypeStruct((n_z, 2 * slots, NS), BF16),
            jax.ShapeDtypeStruct((messages, LANES), BF16),
        ),
        0, 2,
    )(arrived, infos)
    partials = exchanged(copies, "z")
    chosen = vmem_call(
        functools.partial(select_kernel, levels_n),
        jax.ShapeDtypeStruct((lat_block, row_block, LANES), BF16),
        0, 4,
    )(partials, step, picks, base)
    got = exchanged(chosen, ("half", *MA)).reshape(n_half, n_ma, row_block, LANES)
    owned, advected = vmem_call(
        functools.partial(advect_kernel, levels_n, slots),
        (
            jax.ShapeDtypeStruct((row_block, lon_block), F32),
            jax.ShapeDtypeStruct((2, levels_n, 1, NPHI), F32),
        ),
        0, 5,
    )(got, cosines, sines, slope, radius)
    return (owned, jnp.swapaxes(advected, 1, 2))


def solution(mesh):
    parts = Mesh(
        mesh.devices.reshape(HALVES, -1, PAIRS, PAIRS, mesh.shape["ma"] // 8, 2),
        ("half", "z", *MA),
    )
    rad = ("half", "z")
    return jax.shard_map(
        on_device,
        mesh=parts,
        in_specs=(
            P(None, MA, rad, None),
            P(),
            P(MA, rad, None),
            P(),
            P((*rad, *MA), None),
            P((*rad, *MA), None),
        ),
        out_specs=(P(MA, rad), P(None, (*rad, *MA), None, None)),
        check_vma=False,
    )
```
